256 devices in a mesh: freq: 8 (over z_lo, x), panel: 32 (over z_hi, y, core).
Axes of the slice: x: 4, y: 4, z: 8 (z_hi: 4, z_lo: 2; z = z_hi * 2 + z_lo), core: 2. Of those that a mesh axis runs over, the one named last changes fastest.
Arguments:
- recorded: float32 [8, 2, 2048, 2048], P('freq', None, 'panel'), parts along dimension 0, may hold values from -60 to 60
- receiver_kernel: bfloat16 [8, 2, 4095], P('freq'), parts along dimension 0, may hold values from -1.5 to 1.5
- source_kernel: bfloat16 [8, 2, 4095], P('freq'), parts along dimension 0, may hold values from -1.5 to 1.5
Outputs:
- primaries: float32 [8, 2, 2048, 2048], P('freq', None, 'panel'), parts along dimension 0
- multiples: bfloat16 [8, 2, 2048, 2048], P('freq', None, 'panel'), parts along dimension 0
The draws below stay inside these ranges and needn't reach their ends.
There are 8 independent parts, one for each index of `freq`. The reference program is written for one: setup_inputs(seed, part) draws one part's arguments, and reference() takes and returns one part's arrays. A program takes and returns all parts, laid end to end along the dimension named above; each array names one. Nothing has to cross between parts.
All inputs are finite; a program needn't handle non-finite values.
Results may differ from the reference program's by a relative error of at most 0.0057.
Values may be sent and summed in bfloat16 or wider, within the bound.
A program may use at most 320 MiB of HBM per device.

```python
import math
import jax
import jax.numpy as jnp

FREQS = 1
NS = 2048
NR = 2048


def focal_kernel(key, width):
    key_taps, key_phase, key_mag = jax.random.split(key, 3)
    count = 2 * width - 1
    taps = jnp.clip(jax.random.normal(key_taps, (FREQS, 2, count), jnp.float32), -6.0, 6.0)
    taps = taps / jnp.sqrt(2.0 * width)
    phase = jax.random.uniform(key_phase, (FREQS, 1), jnp.float32, -math.pi, math.pi)
    magnitude = jax.random.uniform(key_mag, (FREQS, 1), jnp.float32, 0.8, 1.2)
    center = (jnp.arange(count) == width - 1)[None, :]
    real_part = jnp.where(center, magnitude * jnp.cos(phase), taps[:, 0])
    imag_part = jnp.where(center, magnitude * jnp.sin(phase), taps[:, 1])
    return jnp.stack([real_part, imag_part], axis=1).astype(jnp.bfloat16)


def draw_receiver_kernel(key, part):
    return focal_kernel(jax.random.fold_in(key, 11), NR)


def draw_source_kernel(key, part):
    return focal_kernel(jax.random.fold_in(key, 23), NS)


def draw_recorded(key, part):
    key_base, key_rows, key_cols = jax.random.split(jax.random.fold_in(key, 37), 3)
    rising = 3.0 ** (jnp.arange(NS, dtype=jnp.float32) / (NS - 1))
    base = jnp.clip(jax.random.normal(key_base, (FREQS, 2, NS, NR), jnp.float32), -6.0, 6.0)
    row_scale = jnp.exp(jax.random.uniform(key_rows, (NS,), jnp.float32, math.log(0.7), math.log(1.4)))
    col_scale = jnp.exp(jax.random.uniform(key_cols, (NR,), jnp.float32, math.log(0.7), math.log(1.4)))
    return base * (rising * row_scale)[:, None] * col_scale[None, :]


def setup_inputs(seed: int = 0, part: int = 0) -> dict:
    keys = jax.random.split(jax.random.key(seed), 4)
    part_splits = jax.random.split(jax.random.fold_in(keys[3], part), 4)
    return {
        "recorded": draw_recorded(jax.random.fold_in(jax.random.fold_in(keys[3], part), 71), part),
        "receiver_kernel": draw_receiver_kernel(jax.random.fold_in(jax.random.fold_in(keys[3], part), 71), part),
        "source_kernel": draw_source_kernel(jax.random.fold_in(jax.random.fold_in(keys[3], part), 71), part),
    }


def toeplitz(kernel, width):
    rows = jnp.arange(width, dtype=jnp.int32)[:, None]
    cols = jnp.arange(width, dtype=jnp.int32)[None, :]
    return kernel[:, cols - rows + width - 1]


def complex_dot(left, right):
    real_part = jnp.dot(left[0], right[0], preferred_element_type=jnp.float32) - jnp.dot(left[1], right[1], preferred_element_type=jnp.float32)
    imag_part = jnp.dot(left[0], right[1], preferred_element_type=jnp.float32) + jnp.dot(left[1], right[0], preferred_element_type=jnp.float32)
    return jnp.stack([real_part, imag_part])


def reference(recorded, receiver_kernel, source_kernel):
    prim_list = []
    mult_list = []
    for slot in range(FREQS):
        data = recorded[slot]
        data_b = data.astype(jnp.bfloat16)
        g_recv = toeplitz(receiver_kernel[slot], NR)
        g_src = toeplitz(source_kernel[slot], NS)
        focused = complex_dot(data_b, g_recv).astype(jnp.bfloat16)
        mult = complex_dot(g_src, focused).astype(jnp.bfloat16)
        mfl = mult.astype(jnp.float32)
        num_re = jnp.sum(mfl[0] * data[0] + mfl[1] * data[1])
        num_im = jnp.sum(mfl[0] * data[1] - mfl[1] * data[0])
        den = jnp.sum(mfl[0] * mfl[0] + mfl[1] * mfl[1]) + 1e-6
        fit_re = num_re / den
        fit_im = num_im / den
        prim_re = data[0] - (fit_re * mfl[0] - fit_im * mfl[1])
        prim_im = data[1] - (fit_re * mfl[1] + fit_im * mfl[0])
        prim_list.append(jnp.stack([prim_re, prim_im]))
        mult_list.append(mult)
    return jnp.stack(prim_list), jnp.stack(mult_list)
```

```python
import functools

import jax
import jax.numpy as jnp
from jax import lax
from jax.experimental import pallas as pl
from jax.experimental.pallas import tpu as pltpu
from jax.sharding import PartitionSpec as P

MESH = pl.DeviceIdType.MESH
PANELS = 32
ROWS = 64
WIDTH = PANELS * ROWS
BLOCK = 256
BLOCKS = WIDTH // BLOCK
PER_BLOCK = BLOCK // ROWS
TAPS = 2 * WIDTH
UNITS = 2 * (2 * BLOCKS - 1)
PAIRS = PANELS // 2
STEP_OFFSETS = (4, 3, 5, 2, 6, 1, 7, 0)


def build_operator(taps_ref, oper_ref, index):
    row = taps_ref[pl.ds(index, 1), :]
    skew = pltpu.roll(jnp.broadcast_to(row, (8, TAPS)), 0, 1, stride=1, stride_axis=0)
    for e in range(8):
        low = pltpu.roll(skew, 16 * e + TAPS - 127, 1)
        high = pltpu.roll(skew, (16 * e + 8 + TAPS - 127) % TAPS, 1)
        rows = jnp.concatenate([low, high], axis=0).astype(jnp.bfloat16)
        for u in range(UNITS):
            at = 128 * (UNITS - 1 - u)
            oper_ref[index, 128 * u + 16 * e : 128 * u + 16 * e + 16, :] = rows[:, at : at + 256]


def kernel(
    rec_hbm,
    taps_ref,
    prim_hbm,
    mult_hbm,
    rec,
    oper,
    left,
    left_turned,
    send_a,
    got_a,
    send_b,
    got_b,
    mult,
    prim,
    part_out,
    part_in,
    local_sem,
    send_sem,
    recv_sem,
):
    me = lax.axis_index("panel")
    barrier = pltpu.get_barrier_semaphore()

    def greet(k, carry):
        pl.semaphore_signal(
            barrier, inc=1, device_id={"panel": lax.rem(me + k, PANELS)}, device_id_type=MESH
        )
        return carry

    lax.fori_loop(1, PANELS, greet, 0)
    load = pltpu.make_async_copy(rec_hbm.at[0], rec, local_sem.at[0])
    load.start()

    def build(index, carry):
        build_operator(taps_ref, oper, index)
        return carry

    def exchange(stage, src, dst, sender, receiver):
        return pltpu.make_async_remote_copy(
            src_ref=src.at[receiver],
            dst_ref=dst.at[sender],
            send_sem=send_sem.at[stage, receiver],
            recv_sem=recv_sem.at[stage, sender],
            device_id={"panel": receiver},
            device_id_type=MESH,
        )

    def product(block, first):
        at = pl.multiple_of((BLOCKS - 1 - block) * BLOCK, BLOCK)
        return jnp.dot(
            left[...], oper[first, pl.ds(at, WIDTH), :], preferred_element_type=jnp.float32
        ) + jnp.dot(
            left_turned[...], oper[first + 1, pl.ds(at, WIDTH), :], preferred_element_type=jnp.float32
        )

    def send_block(stage, src, dst, block):
        for h in range(PER_BLOCK):
            target = block * PER_BLOCK + h

            @pl.when(target != me)
            def _():
                exchange(stage, src, dst, me, target).start()

            @pl.when(target == me)
            def _():
                dst[me] = src[me]

    lax.fori_loop(0, 2, build, 0)
    load.wait()
    data_re = rec[0].astype(jnp.bfloat16)
    data_im = rec[1].astype(jnp.bfloat16)
    left[0:ROWS, :] = data_re
    left[ROWS : 2 * ROWS, :] = data_im
    left_turned[0:ROWS, :] = -data_im
    left_turned[ROWS : 2 * ROWS, :] = data_re
    lane = lax.broadcasted_iota(jnp.int32, (ROWS, 128), 1)
    low_half = lane < ROWS
    first_block = me // PER_BLOCK

    def block_of(step):
        half = (step + 1) // 2
        away = jnp.where(lax.rem(step, 2) == 0, BLOCKS // 2 + half, BLOCKS // 2 - half)
        return lax.rem(first_block + away, BLOCKS)

    def forward(step, carry):
        block = block_of(step)
        result = product(block, 0)

        for g in range(2):
            re = result[0:ROWS, 128 * g : 128 * g + 128]
            im = result[ROWS : 2 * ROWS, 128 * g : 128 * g + 128]
            even = jnp.where(low_half, re, pltpu.roll(im, ROWS, 1))
            odd = jnp.where(low_half, pltpu.roll(re, ROWS, 1), im)
            send_a[block * PER_BLOCK + 2 * g] = even.astype(jnp.bfloat16)
            send_a[block * PER_BLOCK + 2 * g + 1] = odd.astype(jnp.bfloat16)

        @pl.when(step == 0)
        def _():
            pl.semaphore_wait(barrier, PANELS - 1)

        send_block(0, send_a, got_a, block)
        return carry

    lax.fori_loop(0, BLOCKS, forward, 0)
    lax.fori_loop(2, 4, build, 0)

    def wait_received(stage, src, dst, sender):
        @pl.when(sender != me)
        def _():
            exchange(stage, src, dst, sender, me).wait_recv()

    def wait_sent(stage, src, dst):
        def one(k, carry):
            exchange(stage, src, dst, me, lax.rem(me + k, PANELS)).wait_send()
            return carry

        lax.fori_loop(1, PANELS, one, 0)

    def turn(pair, carry):
        wait_received(0, send_a, got_a, 2 * pair)
        wait_received(0, send_a, got_a, 2 * pair + 1)
        both = jnp.concatenate([got_a[2 * pair], got_a[2 * pair + 1]], axis=0)
        flipped = both.astype(jnp.float32).T
        at = pl.ds(pl.multiple_of(pair * 128, 128), 128)
        left[:, at] = flipped.astype(jnp.bfloat16)
        left_turned[0:ROWS, at] = (-flipped[ROWS : 2 * ROWS]).astype(jnp.bfloat16)
        left_turned[ROWS : 2 * ROWS, at] = flipped[0:ROWS].astype(jnp.bfloat16)
        return carry

    lax.fori_loop(0, PAIRS, turn, 0)

    def backward(step, carry):
        block = block_of(step)
        result = product(block, 2).T.astype(jnp.bfloat16)
        for h in range(PER_BLOCK):
            send_b[block * PER_BLOCK + h] = result[ROWS * h : ROWS * (h + 1)]
        send_block(1, send_b, got_b, block)
        return carry

    lax.fori_loop(0, BLOCKS, backward, 0)
    wait_sent(0, send_a, got_a)

    def fold(x):
        total = x[0:8]
        for k in range(1, ROWS // 8):
            total = total + x[8 * k : 8 * k + 8]
        return total

    def collect(pair, carry):
        num_re, num_im, energy = carry
        wait_received(1, send_b, got_b, 2 * pair)
        wait_received(1, send_b, got_b, 2 * pair + 1)
        even = got_b[2 * pair].astype(jnp.float32)
        odd = got_b[2 * pair + 1].astype(jnp.float32)
        re = jnp.where(low_half, even, pltpu.roll(odd, ROWS, 1))
        im = jnp.where(low_half, pltpu.roll(even, ROWS, 1), odd)
        at = pl.ds(pl.multiple_of(pair * 128, 128), 128)
        mult[0, :, at] = re.astype(jnp.bfloat16)
        mult[1, :, at] = im.astype(jnp.bfloat16)
        data_re = rec[0, :, at]
        data_im = rec[1, :, at]
        return (
            num_re + fold(re * data_re + im * data_im),
            num_im + fold(re * data_im - im * data_re),
            energy + fold(re * re + im * im),
        )

    zero = jnp.zeros((8, 128), jnp.float32)
    num_re, num_im, energy = lax.fori_loop(0, PAIRS, collect, (zero, zero, zero))
    part_out[0:8] = num_re
    part_out[8:16] = num_im
    part_out[16:24] = energy
    keep = pltpu.make_async_copy(mult, mult_hbm.at[0], local_sem.at[1])
    keep.start()

    def share(k, wait):
        target = lax.rem(me + k, PANELS)
        return pltpu.make_async_remote_copy(
            src_ref=part_out,
            dst_ref=part_in.at[me],
            send_sem=send_sem.at[2, target],
            recv_sem=recv_sem.at[2, me],
            device_id={"panel": target},
            device_id_type=MESH,
        )

    def share_start(k, carry):
        share(k, False).start()
        return carry

    lax.fori_loop(1, PANELS, share_start, 0)
    wait_sent(1, send_b, got_b)

    def gather(k, total):
        sender = lax.rem(me + k, PANELS)
        pltpu.make_async_remote_copy(
            src_ref=part_out,
            dst_ref=part_in.at[sender],
            send_sem=send_sem.at[2, me],
            recv_sem=recv_sem.at[2, sender],
            device_id={"panel": sender},
            device_id_type=MESH,
        ).wait_recv()
        return total + part_in[sender]

    total = lax.fori_loop(1, PANELS, gather, part_out[...])
    sums = [jnp.sum(total[8 * k : 8 * k + 8], keepdims=True) for k in range(3)]
    den = sums[2] + 1e-06
    fit_re = sums[0] / den
    fit_im = sums[1] / den

    def subtract(pair, carry):
        at = pl.ds(pl.multiple_of(pair * 128, 128), 128)
        re = mult[0, :, at].astype(jnp.float32)
        im = mult[1, :, at].astype(jnp.float32)
        prim[0, :, at] = rec[0, :, at] - (fit_re * re - fit_im * im)
        prim[1, :, at] = rec[1, :, at] - (fit_re * im + fit_im * re)
        return carry

    lax.fori_loop(0, PAIRS, subtract, 0)
    store = pltpu.make_async_copy(prim, prim_hbm.at[0], local_sem.at[2])
    store.start()

    def share_done(k, carry):
        share(k, True).wait_send()
        return carry

    lax.fori_loop(1, PANELS, share_done, 0)
    keep.wait()
    store.wait()


def per_device(recorded, receiver_kernel, source_kernel):
    taps = jnp.concatenate([receiver_kernel[0], jnp.flip(source_kernel[0], axis=1)], axis=0)
    taps = jnp.pad(taps.astype(jnp.float32), ((0, 4), (0, 1)))
    vmem = pltpu.VMEM
    return pl.pallas_call(
        kernel,
        out_shape=(
            jax.ShapeDtypeStruct((1, 2, ROWS, WIDTH), jnp.float32),
            jax.ShapeDtypeStruct((1, 2, ROWS, WIDTH), jnp.bfloat16),
        ),
        in_specs=[
            pl.BlockSpec(memory_space=pl.ANY),
            pl.BlockSpec(memory_space=pltpu.VMEM),
        ],
        out_specs=(
            pl.BlockSpec(memory_space=pl.ANY),
            pl.BlockSpec(memory_space=pl.ANY),
        ),
        scratch_shapes=[
            vmem((2, ROWS, WIDTH), jnp.float32),
            vmem((4, 128 * UNITS, BLOCK), jnp.bfloat16),
            vmem((2 * ROWS, WIDTH), jnp.bfloat16),
            vmem((2 * ROWS, WIDTH), jnp.bfloat16),
            vmem((PANELS, ROWS, 128), jnp.bfloat16),
            vmem((PANELS, ROWS, 128), jnp.bfloat16),
            vmem((PANELS, ROWS, 128), jnp.bfloat16),
            vmem((PANELS, ROWS, 128), jnp.bfloat16),
            vmem((2, ROWS, WIDTH), jnp.bfloat16),
            vmem((2, ROWS, WIDTH), jnp.float32),
            vmem((24, 128), jnp.float32),
            vmem((PANELS, 24, 128), jnp.float32),
            pltpu.SemaphoreType.DMA((3,)),
            pltpu.SemaphoreType.DMA((3, PANELS)),
            pltpu.SemaphoreType.DMA((3, PANELS)),
        ],
        compiler_params=pltpu.CompilerParams(
            collective_id=0, has_side_effects=True, vmem_limit_bytes=48 * 1024 * 1024
        ),
    )(recorded, taps)


def solution(mesh):
    placed = (P("freq", None, "panel", None), P("freq", None, None), P("freq", None, None))
    return jax.shard_map(
        per_device,
        mesh=mesh,
        in_specs=placed,
        out_specs=(P("freq", None, "panel", None), P("freq", None, "panel", None)),
        check_vma=False,
    )
```

```python
import functools

import jax
import jax.numpy as jnp
from jax import lax
from jax.experimental import pallas as pl
from jax.experimental.pallas import tpu as pltpu
from jax.sharding import PartitionSpec as P

MESH = pl.DeviceIdType.MESH
PANELS = 32
ROWS = 64
WIDTH = PANELS * ROWS
BLOCK = 256
BLOCKS = WIDTH // BLOCK
PER_BLOCK = BLOCK // ROWS
TAPS = 2 * WIDTH
UNITS = 2 * (2 * BLOCKS - 1)
PAIRS = PANELS // 2


def build_operator(taps_ref, oper_ref, index):
    row = taps_ref[pl.ds(index, 1), :]
    skew = pltpu.roll(jnp.broadcast_to(row, (8, TAPS)), 0, 1, stride=1, stride_axis=0)
    for e in range(8):
        low = pltpu.roll(skew, 16 * e + TAPS - 128, 1)
        high = pltpu.roll(skew, 16 * e + 8 + TAPS - 128, 1)
        rows = jnp.concatenate([low, high], axis=0).astype(jnp.bfloat16)
        for u in range(UNITS):
            at = 128 * (UNITS - 1 - u)
            oper_ref[index, 128 * u + 16 * e : 128 * u + 16 * e + 16, :] = rows[:, at : at + 256]


def kernel(
    rec_hbm,
    receiver_hbm,
    source_hbm,
    prim,
    mult,
    rec,
    raw,
    taps_ref,
    oper,
    left,
    left_turned,
    send_a,
    got_a,
    send_b,
    got_b,
    part_out,
    part_in,
    local_sem,
    send_sem,
    recv_sem,
):
    me = lax.axis_index("panel")
    barrier = pltpu.get_barrier_semaphore()

    def greet(k, carry):
        pl.semaphore_signal(
            barrier, inc=1, device_id={"panel": lax.rem(me + k, PANELS)}, device_id_type=MESH
        )
        return carry

    lax.fori_loop(1, PANELS, greet, 0)
    loads = [
        pltpu.make_async_copy(receiver_hbm.at[0], raw.at[0], local_sem.at[0]),
        pltpu.make_async_copy(source_hbm.at[0], raw.at[1], local_sem.at[1]),
        pltpu.make_async_copy(rec_hbm.at[0], rec, local_sem.at[2]),
    ]
    for load in loads:
        load.start()

    def build(index, carry):
        build_operator(taps_ref, oper, index)
        return carry

    def exchange(stage, src, dst, sender, receiver):
        return pltpu.make_async_remote_copy(
            src_ref=src.at[receiver],
            dst_ref=dst.at[sender],
            send_sem=send_sem.at[stage, receiver],
            recv_sem=recv_sem.at[stage, sender],
            device_id={"panel": receiver},
            device_id_type=MESH,
        )

    def product(block, first):
        at = pl.multiple_of((BLOCKS - 1 - block) * BLOCK, BLOCK)
        return jnp.dot(
            left[...], oper[first, pl.ds(at, WIDTH), :], preferred_element_type=jnp.float32
        ) + jnp.dot(
            left_turned[...], oper[first + 1, pl.ds(at, WIDTH), :], preferred_element_type=jnp.float32
        )

    def send_block(stage, src, dst, block):
        for h in range(PER_BLOCK):
            target = block * PER_BLOCK + h

            @pl.when(target != me)
            def _():
                exchange(stage, src, dst, me, target).start()

            @pl.when(target == me)
            def _():
                dst[me] = src[me]

    loads[0].wait()
    taps_ref[...] = jnp.zeros_like(taps_ref)
    taps_ref[0:2, 0 : TAPS - 1] = raw[0].astype(jnp.float32)
    taps_ref[0:2, :] = pltpu.roll(taps_ref[0:8, :], 1, 1)[0:2]
    lax.fori_loop(0, 2, build, 0)
    loads[2].wait()
    data_re = rec[0].astype(jnp.bfloat16)
    data_im = rec[1].astype(jnp.bfloat16)
    left[0:ROWS, :] = data_re
    left[ROWS : 2 * ROWS, :] = data_im
    left_turned[0:ROWS, :] = -data_im
    left_turned[ROWS : 2 * ROWS, :] = data_re
    lane = lax.broadcasted_iota(jnp.int32, (ROWS, 128), 1)
    low_half = lane < ROWS
    first_block = me // PER_BLOCK

    def block_of(step):
        half = (step + 1) // 2
        away = jnp.where(lax.rem(step, 2) == 0, BLOCKS // 2 + half, BLOCKS // 2 - half)
        return lax.rem(first_block + away, BLOCKS)

    def forward(step, carry):
        block = block_of(step)
        result = product(block, 0)

        for g in range(2):
            re = result[0:ROWS, 128 * g : 128 * g + 128]
            im = result[ROWS : 2 * ROWS, 128 * g : 128 * g + 128]
            even = jnp.where(low_half, re, pltpu.roll(im, ROWS, 1))
            odd = jnp.where(low_half, pltpu.roll(re, ROWS, 1), im)
            send_a[block * PER_BLOCK + 2 * g] = even.astype(jnp.bfloat16)
            send_a[block * PER_BLOCK + 2 * g + 1] = odd.astype(jnp.bfloat16)

        @pl.when(step == 0)
        def _():
            pl.semaphore_wait(barrier, PANELS - 1)

        send_block(0, send_a, got_a, block)
        return carry

    lax.fori_loop(0, BLOCKS, forward, 0)
    loads[1].wait()
    taps_ref[8:10, 0 : TAPS - 1] = raw[1].astype(jnp.float32)
    mirror = (
        lax.broadcasted_iota(jnp.int32, (128, 128), 0)
        + lax.broadcasted_iota(jnp.int32, (128, 128), 1)
        == 127
    ).astype(jnp.bfloat16)
    for g in range(TAPS // 128):
        piece = taps_ref[8:16, 128 * g : 128 * g + 128].astype(jnp.bfloat16)
        turned = jnp.dot(piece, mirror, preferred_element_type=jnp.float32)
        taps_ref[2:4, TAPS - 128 * (g + 1) : TAPS - 128 * g] = turned[0:2]
    lax.fori_loop(2, 4, build, 0)

    def wait_received(stage, src, dst, sender):
        @pl.when(sender != me)
        def _():
            exchange(stage, src, dst, sender, me).wait_recv()

    def wait_sent(stage, src, dst):
        def one(k, carry):
            exchange(stage, src, dst, me, lax.rem(me + k, PANELS)).wait_send()
            return carry

        lax.fori_loop(1, PANELS, one, 0)

    def turn(pair, carry):
        wait_received(0, send_a, got_a, 2 * pair)
        wait_received(0, send_a, got_a, 2 * pair + 1)
        both = jnp.concatenate([got_a[2 * pair], got_a[2 * pair + 1]], axis=0)
        flipped = both.astype(jnp.float32).T
        at = pl.ds(pl.multiple_of(pair * 128, 128), 128)
        left[:, at] = flipped.astype(jnp.bfloat16)
        left_turned[0:ROWS, at] = (-flipped[ROWS : 2 * ROWS]).astype(jnp.bfloat16)
        left_turned[ROWS : 2 * ROWS, at] = flipped[0:ROWS].astype(jnp.bfloat16)
        return carry

    lax.fori_loop(0, PAIRS, turn, 0)

    def backward(step, carry):
        block = block_of(step)
        result = product(block, 2).T.astype(jnp.bfloat16)
        for h in range(PER_BLOCK):
            send_b[block * PER_BLOCK + h] = result[ROWS * h : ROWS * (h + 1)]
        send_block(1, send_b, got_b, block)
        return carry

    lax.fori_loop(0, BLOCKS, backward, 0)
    wait_sent(0, send_a, got_a)

    def fold(x):
        total = x[0:8]
        for k in range(1, ROWS // 8):
            total = total + x[8 * k : 8 * k + 8]
        return total

    def collect(pair, carry):
        num_re, num_im, energy = carry
        wait_received(1, send_b, got_b, 2 * pair)
        wait_received(1, send_b, got_b, 2 * pair + 1)
        even = got_b[2 * pair].astype(jnp.float32)
        odd = got_b[2 * pair + 1].astype(jnp.float32)
        re = jnp.where(low_half, even, pltpu.roll(odd, ROWS, 1))
        im = jnp.where(low_half, pltpu.roll(even, ROWS, 1), odd)
        at = pl.ds(pl.multiple_of(pair * 128, 128), 128)
        mult[0, 0, :, at] = re.astype(jnp.bfloat16)
        mult[0, 1, :, at] = im.astype(jnp.bfloat16)
        data_re = rec[0, :, at]
        data_im = rec[1, :, at]
        return (
            num_re + fold(re * data_re + im * data_im),
            num_im + fold(re * data_im - im * data_re),
            energy + fold(re * re + im * im),
        )

    zero = jnp.zeros((8, 128), jnp.float32)
    num_re, num_im, energy = lax.fori_loop(0, PAIRS, collect, (zero, zero, zero))
    part_out[0:8] = num_re
    part_out[8:16] = num_im
    part_out[16:24] = energy

    def share(k, wait):
        target = lax.rem(me + k, PANELS)
        return pltpu.make_async_remote_copy(
            src_ref=part_out,
            dst_ref=part_in.at[me],
            send_sem=send_sem.at[2, target],
            recv_sem=recv_sem.at[2, me],
            device_id={"panel": target},
            device_id_type=MESH,
        )

    def share_start(k, carry):
        share(k, False).start()
        return carry

    lax.fori_loop(1, PANELS, share_start, 0)
    wait_sent(1, send_b, got_b)

    def gather(k, total):
        sender = lax.rem(me + k, PANELS)
        pltpu.make_async_remote_copy(
            src_ref=part_out,
            dst_ref=part_in.at[sender],
            send_sem=send_sem.at[2, me],
            recv_sem=recv_sem.at[2, sender],
            device_id={"panel": sender},
            device_id_type=MESH,
        ).wait_recv()
        return total + part_in[sender]

    total = lax.fori_loop(1, PANELS, gather, part_out[...])
    sums = [jnp.sum(total[8 * k : 8 * k + 8], keepdims=True) for k in range(3)]
    den = sums[2] + 1e-06
    fit_re = sums[0] / den
    fit_im = sums[1] / den

    def subtract(pair, carry):
        at = pl.ds(pl.multiple_of(pair * 128, 128), 128)
        re = mult[0, 0, :, at].astype(jnp.float32)
        im = mult[0, 1, :, at].astype(jnp.float32)
        prim[0, 0, :, at] = rec[0, :, at] - (fit_re * re - fit_im * im)
        prim[0, 1, :, at] = rec[1, :, at] - (fit_re * im + fit_im * re)
        return carry

    lax.fori_loop(0, PAIRS, subtract, 0)

    def share_done(k, carry):
        share(k, True).wait_send()
        return carry

    lax.fori_loop(1, PANELS, share_done, 0)


def per_device(recorded, receiver_kernel, source_kernel):
    vmem = pltpu.VMEM
    return pl.pallas_call(
        kernel,
        out_shape=(
            jax.ShapeDtypeStruct((1, 2, ROWS, WIDTH), jnp.float32),
            jax.ShapeDtypeStruct((1, 2, ROWS, WIDTH), jnp.bfloat16),
        ),
        in_specs=[
            pl.BlockSpec(memory_space=pltpu.HBM),
            pl.BlockSpec(memory_space=pltpu.HBM),
            pl.BlockSpec(memory_space=pltpu.HBM),
        ],
        out_specs=(
            pl.BlockSpec(memory_space=pltpu.VMEM),
            pl.BlockSpec(memory_space=pltpu.VMEM),
        ),
        scratch_shapes=[
            vmem((2, ROWS, WIDTH), jnp.float32),
            vmem((2, 2, TAPS - 1), jnp.bfloat16),
            vmem((16, TAPS), jnp.float32),
            vmem((4, 128 * UNITS, BLOCK), jnp.bfloat16),
            vmem((2 * ROWS, WIDTH), jnp.bfloat16),
            vmem((2 * ROWS, WIDTH), jnp.bfloat16),
            vmem((PANELS, ROWS, 128), jnp.bfloat16),
            vmem((PANELS, ROWS, 128), jnp.bfloat16),
            vmem((PANELS, ROWS, 128), jnp.bfloat16),
            vmem((PANELS, ROWS, 128), jnp.bfloat16),
            vmem((24, 128), jnp.float32),
            vmem((PANELS, 24, 128), jnp.float32),
            pltpu.SemaphoreType.DMA((3,)),
            pltpu.SemaphoreType.DMA((3, PANELS)),
            pltpu.SemaphoreType.DMA((3, PANELS)),
        ],
        compiler_params=pltpu.CompilerParams(
            collective_id=0, has_side_effects=True, vmem_limit_bytes=48 * 1024 * 1024
        ),
    )(recorded, receiver_kernel, source_kernel)


def solution(mesh):
    placed = (P("freq", None, "panel", None), P("freq", None, None), P("freq", None, None))
    return jax.shard_map(
        per_device,
        mesh=mesh,
        in_specs=placed,
        out_specs=(P("freq", None, "panel", None), P("freq", None, "panel", None)),
        check_vma=False,
    )
```

```python
import jax
import jax.numpy as jnp
from jax import lax
from jax.experimental import pallas as pl
from jax.experimental.pallas import tpu as pltpu
from jax.sharding import PartitionSpec as P

MESH = pl.DeviceIdType.MESH
PANELS = 32
ROWS = 64
WIDTH = PANELS * ROWS
BLOCK = 256
BLOCKS = WIDTH // BLOCK
TAPS = 2 * WIDTH
UNITS = 2 * (2 * BLOCKS - 1)
CHUNKS = 2
SUB = ROWS // CHUNKS
HALF = WIDTH // 2
GROUP = 8
GROUPS = PANELS // GROUP


def rolled_taps(taps_ref, index, e):
    skew = pltpu.roll(
        jnp.broadcast_to(taps_ref[pl.ds(index, 1), :], (8, TAPS)), 0, 1, stride=1, stride_axis=0
    )
    low = pltpu.roll(skew, 16 * e + TAPS - 128, 1)
    high = pltpu.roll(skew, 16 * e + 8 + TAPS - 128, 1)
    return jnp.concatenate([low, high], axis=0).astype(jnp.bfloat16)


def spread(parts, quarter):
    outs = []
    for i in range(4):
        out = parts[i]
        for k in range(4):
            if k != i:
                out = jnp.where(quarter == k, pltpu.roll(parts[k], 32 * (k - i) % 128, 1), out)
        outs.append(out)
    return outs


def kernel(
    rec,
    receiver_taps,
    source_taps,
    prim,
    mult,
    taps_ref,
    oper,
    skewed,
    mixed,
    left,
    left_turned,
    half,
    half_turned,
    send_a,
    got_a,
    send_b,
    got_b,
    part_out,
    part_in,
    send_sem,
    recv_sem,
):
    me = lax.axis_index("panel")
    my_group, my_seat = me // GROUP, lax.rem(me, GROUP)
    barrier = pltpu.get_barrier_semaphore()

    def greet(k, carry):
        pl.semaphore_signal(
            barrier, inc=1, device_id={"panel": lax.rem(me + k, PANELS)}, device_id_type=MESH
        )
        return carry

    lax.fori_loop(1, PANELS, greet, 0)

    def exchange(stage, src, dst, chunk, target):
        return pltpu.make_async_remote_copy(
            src_ref=src.at[chunk, target],
            dst_ref=dst.at[chunk, me],
            send_sem=send_sem.at[stage, chunk],
            recv_sem=recv_sem.at[stage, chunk],
            device_id={"panel": target},
            device_id_type=MESH,
        )

    def whole(stage, src, dst, chunk):
        others = pl.ds(0, PANELS - 1)
        return pltpu.make_async_remote_copy(
            src_ref=src.at[chunk, others],
            dst_ref=dst.at[chunk, others],
            send_sem=send_sem.at[stage, chunk],
            recv_sem=recv_sem.at[stage, chunk],
            device_id={"panel": lax.rem(me + 1, PANELS)},
            device_id_type=MESH,
        )

    def post(stage, src, dst, chunk, target):
        @pl.when(target != me)
        def _():
            exchange(stage, src, dst, chunk, target).start()

        @pl.when(target == me)
        def _():
            dst[chunk, me] = src[chunk, me]

    taps_ref[...] = jnp.zeros_like(taps_ref)
    taps_ref[0:2, 0 : TAPS - 1] = receiver_taps[0].astype(jnp.float32)
    taps_ref[0:2, :] = pltpu.roll(taps_ref[0:8, :], 1, 1)[0:2]

    def build_receiver(index, carry):
        for e in range(8):
            rows = rolled_taps(taps_ref, index, e)
            for u in range(UNITS):
                at = 128 * (UNITS - 1 - u)
                oper[index, 128 * u + 16 * e : 128 * u + 16 * e + 16, :] = rows[:, at : at + 256]
        return carry

    lax.fori_loop(0, 2, build_receiver, 0)
    data_re = rec[0, 0].astype(jnp.bfloat16)
    data_im = rec[0, 1].astype(jnp.bfloat16)
    left[0:ROWS, :] = data_re
    left[ROWS : 2 * ROWS, :] = data_im
    left_turned[0:ROWS, :] = -data_im
    left_turned[ROWS : 2 * ROWS, :] = data_re
    quarter = lax.broadcasted_iota(jnp.int32, (SUB, 128), 1) // 32

    def forward(step, carry):
        chunk, turn = step // GROUPS, lax.rem(step, GROUPS)
        shift = (turn + 1) // 2
        away = jnp.where(lax.rem(turn, 2) == 0, GROUPS // 2 + shift, GROUPS // 2 - shift)
        group = lax.rem(my_group + away, GROUPS)
        at = pl.multiple_of((BLOCKS - 1 - chunk * GROUPS - group) * BLOCK, BLOCK)
        result = jnp.dot(
            left[...], oper[0, pl.ds(at, WIDTH), :], preferred_element_type=jnp.float32
        ) + jnp.dot(
            left_turned[...], oper[1, pl.ds(at, WIDTH), :], preferred_element_type=jnp.float32
        )
        for g in range(2):
            lanes = slice(128 * g, 128 * g + 128)
            parts = [
                result[ROWS * comp + SUB * h : ROWS * comp + SUB * h + SUB, lanes]
                for h in range(2)
                for comp in range(2)
            ]
            for i, out in enumerate(spread(parts, quarter)):
                send_a[chunk, group * GROUP + 4 * g + i] = out.astype(jnp.bfloat16)

        @pl.when(step == 0)
        def _():
            pl.semaphore_wait(barrier, PANELS - 1)

        def one(t, inner):
            post(0, send_a, got_a, chunk, group * GROUP + lax.rem(my_seat + t, GROUP))
            return inner

        lax.fori_loop(0, GROUP, one, 0)
        return carry

    lax.fori_loop(0, BLOCKS, forward, 0)

    taps_ref[8:10, 0 : TAPS - 1] = source_taps[0].astype(jnp.float32)
    mirror = (
        lax.broadcasted_iota(jnp.int32, (128, 128), 0)
        + lax.broadcasted_iota(jnp.int32, (128, 128), 1)
        == 127
    ).astype(jnp.bfloat16)
    for g in range(TAPS // 128):
        piece = taps_ref[8:16, 128 * g : 128 * g + 128].astype(jnp.bfloat16)
        turned = jnp.dot(piece, mirror, preferred_element_type=jnp.float32)
        taps_ref[2:4, TAPS - 128 * (g + 1) : TAPS - 128 * g] = turned[0:2]
    narrow = lax.broadcasted_iota(jnp.int32, (16, 128), 1) // 32

    def build_source(comp, carry):
        for e in range(8):
            skewed[16 * e : 16 * e + 16, :] = rolled_taps(taps_ref, 2 + comp, e)

        def unit(u, inner):
            for e in range(8):
                to = pl.ds(pl.multiple_of(64 * u + 32 * (e // 4) + 16 * (e % 2), 16), 16)
                for h in range(2):
                    out = None
                    for i in range(4):
                        back = 2 * (i + h)
                        tile = UNITS - 1 - u + (1 if e < back else 0)
                        row = 16 * ((e - back) % 8)
                        piece = skewed[row : row + 16, pl.ds(pl.multiple_of(tile * 128, 128), 128)]
                        piece = piece.astype(jnp.float32)
                        out = piece if out is None else jnp.where(narrow == i, piece, out)
                    mixed[comp, (e // 2) % 2, to, 128 * h : 128 * h + 128] = out.astype(jnp.bfloat16)
            return inner

        lax.fori_loop(0, UNITS, unit, 0)
        return carry

    lax.fori_loop(0, 2, build_source, 0)
    first_block = me // 4

    def second(chunk, carry):
        whole(0, send_a, got_a, chunk).wait_recv()

        def turn(g, inner):
            block = jnp.concatenate([got_a[chunk, 4 * g + i] for i in range(4)], axis=0)
            flipped = block.astype(jnp.float32).T
            at = pl.ds(pl.multiple_of(g * 128, 128), 128)
            for h in range(2):
                re = flipped[2 * SUB * h : 2 * SUB * h + SUB]
                im = flipped[2 * SUB * h + SUB : 2 * SUB * (h + 1)]
                half[h, 0:SUB, at] = re.astype(jnp.bfloat16)
                half[h, SUB : 2 * SUB, at] = im.astype(jnp.bfloat16)
                half_turned[h, 0:SUB, at] = (-im).astype(jnp.bfloat16)
                half_turned[h, SUB : 2 * SUB, at] = re.astype(jnp.bfloat16)
            return inner

        lax.fori_loop(0, PANELS // 4, turn, 0)

        def backward(step, inner):
            shift = (step + 1) // 2
            away = jnp.where(lax.rem(step, 2) == 0, BLOCKS // 2 + shift, BLOCKS // 2 - shift)
            block = lax.rem(first_block + away, BLOCKS)
            at = pl.ds(pl.multiple_of((BLOCKS - 1 - block) * 128, 128), HALF)
            result = None
            for h in range(2):
                for comp, lhs in enumerate((half, half_turned)):
                    term = jnp.dot(lhs[h], mixed[comp, h, at, :], preferred_element_type=jnp.float32)
                    result = term if result is None else result + term
            stacked = jnp.concatenate([result[:, 0:128], result[:, 128:256]], axis=0)
            rows = stacked.T.astype(jnp.bfloat16)
            for i in range(4):
                send_b[chunk, block * 4 + i] = rows[SUB * i : SUB * i + SUB]
                post(1, send_b, got_b, chunk, block * 4 + i)
            return inner

        lax.fori_loop(0, BLOCKS, backward, 0)
        return carry

    lax.fori_loop(0, CHUNKS, second, 0)

    def fold(x):
        total = x[0:8]
        for k in range(1, SUB // 8):
            total = total + x[8 * k : 8 * k + 8]
        return total

    def collect(chunk, sums):
        whole(1, send_b, got_b, chunk).wait_recv()

        def tile(g, sums):
            parts = [got_b[chunk, 4 * g + i].astype(jnp.float32) for i in range(4)]
            outs = spread(parts, quarter)
            at = pl.ds(pl.multiple_of(chunk * HALF + g * 128, 128), 128)
            num_re, num_im, energy = sums
            for h in range(2):
                re, im = outs[2 * h], outs[2 * h + 1]
                rows = slice(SUB * h, SUB * h + SUB)
                mult[0, 0, rows, at] = re.astype(jnp.bfloat16)
                mult[0, 1, rows, at] = im.astype(jnp.bfloat16)
                data_re = rec[0, 0, rows, at]
                data_im = rec[0, 1, rows, at]
                num_re = num_re + fold(re * data_re + im * data_im)
                num_im = num_im + fold(re * data_im - im * data_re)
                energy = energy + fold(re * re + im * im)
            return num_re, num_im, energy

        return lax.fori_loop(0, PANELS // 4, tile, sums)

    zero = jnp.zeros((8, 128), jnp.float32)
    sums = lax.fori_loop(0, CHUNKS, collect, (zero, zero, zero))
    column = lax.broadcasted_iota(jnp.int32, (1, 128), 1)
    sums = [jnp.sum(x, keepdims=True) for x in sums]
    mine = jnp.where(column == 0, sums[0], jnp.where(column == 1, sums[1], sums[2]))
    part_out[0:1, 0:1] = mine[None]
    part_in[pl.ds(me, 1), 0:1] = mine[None]

    def share(k, carry):
        target = lax.rem(me + k, PANELS)
        pltpu.make_async_remote_copy(
            src_ref=part_out.at[pl.ds(0, 1), pl.ds(0, 1)],
            dst_ref=part_in.at[pl.ds(me, 1), pl.ds(0, 1)],
            send_sem=send_sem.at[2, 0],
            recv_sem=recv_sem.at[2, 0],
            device_id={"panel": target},
            device_id_type=MESH,
        ).start()
        return carry

    lax.fori_loop(1, PANELS, share, 0)
    for chunk in range(CHUNKS):
        whole(0, send_a, got_a, chunk).wait_send()
        whole(1, send_b, got_b, chunk).wait_send()
    others = pl.ds(0, PANELS - 1)
    shared = pltpu.make_async_remote_copy(
        src_ref=part_in.at[others, pl.ds(0, 1)],
        dst_ref=part_in.at[others, pl.ds(0, 1)],
        send_sem=send_sem.at[2, 0],
        recv_sem=recv_sem.at[2, 0],
        device_id={"panel": lax.rem(me + 1, PANELS)},
        device_id_type=MESH,
    )
    shared.wait_recv()
    total = part_in[0, 0:1]
    for k in range(1, PANELS):
        total = total + part_in[k, 0:1]
    den = total[:, 2:3] + 1e-06
    fit_re = total[:, 0:1] / den
    fit_im = total[:, 1:2] / den

    def subtract(pair, carry):
        at = pl.ds(pl.multiple_of(pair * 128, 128), 128)
        re = mult[0, 0, :, at].astype(jnp.float32)
        im = mult[0, 1, :, at].astype(jnp.float32)
        prim[0, 0, :, at] = rec[0, 0, :, at] - (fit_re * re - fit_im * im)
        prim[0, 1, :, at] = rec[0, 1, :, at] - (fit_re * im + fit_im * re)
        return carry

    lax.fori_loop(0, WIDTH // 128, subtract, 0)
    shared.wait_send()


def per_device(recorded, receiver_kernel, source_kernel):
    vmem = pltpu.VMEM
    bf16 = jnp.bfloat16
    return pl.pallas_call(
        kernel,
        out_shape=(
            jax.ShapeDtypeStruct((1, 2, ROWS, WIDTH), jnp.float32),
            jax.ShapeDtypeStruct((1, 2, ROWS, WIDTH), bf16),
        ),
        in_specs=[pl.BlockSpec(memory_space=vmem)] * 3,
        out_specs=(pl.BlockSpec(memory_space=vmem), pl.BlockSpec(memory_space=vmem)),
        scratch_shapes=[
            vmem((16, TAPS), jnp.float32),
            vmem((2, 128 * UNITS, BLOCK), bf16),
            vmem((128, TAPS), bf16),
            vmem((2, 2, 64 * UNITS, BLOCK), bf16),
            vmem((2 * ROWS, WIDTH), bf16),
            vmem((2 * ROWS, WIDTH), bf16),
            vmem((2, 2 * SUB, HALF), bf16),
            vmem((2, 2 * SUB, HALF), bf16),
            vmem((CHUNKS, PANELS, SUB, 128), bf16),
            vmem((CHUNKS, PANELS, SUB, 128), bf16),
            vmem((CHUNKS, PANELS, SUB, 128), bf16),
            vmem((CHUNKS, PANELS, SUB, 128), bf16),
            vmem((1, 8, 128), jnp.float32),
            vmem((PANELS, 8, 128), jnp.float32),
            pltpu.SemaphoreType.DMA((3, CHUNKS)),
            pltpu.SemaphoreType.DMA((3, CHUNKS)),
        ],
        compiler_params=pltpu.CompilerParams(
            collective_id=0, has_side_effects=True, vmem_limit_bytes=48 * 1024 * 1024
        ),
    )(recorded, receiver_kernel, source_kernel)


def solution(mesh):
    placed = (P("freq", None, "panel", None), P("freq", None, None), P("freq", None, None))
    return jax.shard_map(
        per_device,
        mesh=mesh,
        in_specs=placed,
        out_specs=(P("freq", None, "panel", None), P("freq", None, "panel", None)),
        check_vma=False,
    )
```

```python
import jax
import jax.numpy as jnp
from jax import lax
from jax.experimental import pallas as pl
from jax.experimental.pallas import tpu as pltpu
from jax.sharding import PartitionSpec as P

MESH = pl.DeviceIdType.MESH
PANELS = 32
ROWS = 64
WIDTH = PANELS * ROWS
BLOCK = 256
BLOCKS = WIDTH // BLOCK
TAPS = 2 * WIDTH
UNITS = 2 * (2 * BLOCKS - 1)
CHUNKS = 2
SUB = ROWS // CHUNKS
HALF = WIDTH // 2
GROUP = 8
GROUPS = PANELS // GROUP


def rolled_taps(taps_ref, index, e):
    skew = pltpu.roll(
        jnp.broadcast_to(taps_ref[pl.ds(index, 1), :], (8, TAPS)), 0, 1, stride=1, stride_axis=0
    )
    low = pltpu.roll(skew, 16 * e + TAPS - 128, 1)
    high = pltpu.roll(skew, 16 * e + 8 + TAPS - 128, 1)
    return jnp.concatenate([low, high], axis=0).astype(jnp.bfloat16)


def spread(parts, quarter):
    outs = []
    for i in range(4):
        out = parts[i]
        for k in range(4):
            if k != i:
                out = jnp.where(quarter == k, pltpu.roll(parts[k], 32 * (k - i) % 128, 1), out)
        outs.append(out)
    return outs


def kernel(
    rec_hbm,
    receiver_hbm,
    source_hbm,
    prim,
    mult,
    rec,
    raw,
    taps_ref,
    oper,
    skewed,
    mixed,
    left,
    left_turned,
    half,
    half_turned,
    send_a,
    got_a,
    send_b,
    got_b,
    part_out,
    part_in,
    load_sem,
    send_sem,
    recv_sem,
):
    me = lax.axis_index("panel")
    my_group, my_seat = me // GROUP, lax.rem(me, GROUP)
    barrier = pltpu.get_barrier_semaphore()

    def greet(k, carry):
        pl.semaphore_signal(
            barrier, inc=1, device_id={"panel": lax.rem(me + k, PANELS)}, device_id_type=MESH
        )
        return carry

    loads = [
        pltpu.make_async_copy(receiver_hbm, raw.at[pl.ds(0, 1)], load_sem.at[0]),
        pltpu.make_async_copy(rec_hbm, rec, load_sem.at[1]),
        pltpu.make_async_copy(source_hbm, raw.at[pl.ds(1, 1)], load_sem.at[2]),
    ]
    for load in loads:
        load.start()
    lax.fori_loop(1, PANELS, greet, 0)

    def exchange(stage, src, dst, chunk, target):
        return pltpu.make_async_remote_copy(
            src_ref=src.at[chunk, target],
            dst_ref=dst.at[chunk, me],
            send_sem=send_sem.at[stage, chunk],
            recv_sem=recv_sem.at[stage, chunk],
            device_id={"panel": target},
            device_id_type=MESH,
        )

    def whole(stage, src, dst, chunk):
        others = pl.ds(0, PANELS - 1)
        return pltpu.make_async_remote_copy(
            src_ref=src.at[chunk, others],
            dst_ref=dst.at[chunk, others],
            send_sem=send_sem.at[stage, chunk],
            recv_sem=recv_sem.at[stage, chunk],
            device_id={"panel": lax.rem(me + 1, PANELS)},
            device_id_type=MESH,
        )

    def post(stage, src, dst, chunk, target):
        @pl.when(target != me)
        def _():
            exchange(stage, src, dst, chunk, target).start()

        @pl.when(target == me)
        def _():
            dst[chunk, me] = src[chunk, me]

    taps_ref[...] = jnp.zeros_like(taps_ref)
    loads[0].wait()
    taps_ref[0:2, 0 : TAPS - 1] = raw[0].astype(jnp.float32)
    taps_ref[0:2, :] = pltpu.roll(taps_ref[0:8, :], 1, 1)[0:2]

    def build_receiver(index, carry):
        for e in range(8):
            rows = rolled_taps(taps_ref, index, e)
            for u in range(UNITS):
                at = 128 * (UNITS - 1 - u)
                oper[index, 128 * u + 16 * e : 128 * u + 16 * e + 16, :] = rows[:, at : at + 256]
        return carry

    lax.fori_loop(0, 2, build_receiver, 0)
    loads[1].wait()
    data_re = rec[0, 0].astype(jnp.bfloat16)
    data_im = rec[0, 1].astype(jnp.bfloat16)
    left[0:ROWS, :] = data_re
    left[ROWS : 2 * ROWS, :] = data_im
    left_turned[0:ROWS, :] = -data_im
    left_turned[ROWS : 2 * ROWS, :] = data_re
    quarter = lax.broadcasted_iota(jnp.int32, (SUB, 128), 1) // 32

    def forward(step, carry):
        chunk, turn = step // GROUPS, lax.rem(step, GROUPS)
        shift = (turn + 1) // 2
        away = jnp.where(lax.rem(turn, 2) == 0, GROUPS // 2 + shift, GROUPS // 2 - shift)
        group = lax.rem(my_group + away, GROUPS)
        at = pl.multiple_of((BLOCKS - 1 - chunk * GROUPS - group) * BLOCK, BLOCK)
        result = jnp.dot(
            left[...], oper[0, pl.ds(at, WIDTH), :], preferred_element_type=jnp.float32
        ) + jnp.dot(
            left_turned[...], oper[1, pl.ds(at, WIDTH), :], preferred_element_type=jnp.float32
        )
        for g in range(2):
            lanes = slice(128 * g, 128 * g + 128)
            parts = [
                result[ROWS * comp + SUB * h : ROWS * comp + SUB * h + SUB, lanes]
                for h in range(2)
                for comp in range(2)
            ]
            for i, out in enumerate(spread(parts, quarter)):
                send_a[chunk, group * GROUP + 4 * g + i] = out.astype(jnp.bfloat16)

        @pl.when(step == 0)
        def _():
            pl.semaphore_wait(barrier, PANELS - 1)

        def one(t, inner):
            post(0, send_a, got_a, chunk, group * GROUP + lax.rem(my_seat + t, GROUP))
            return inner

        lax.fori_loop(0, GROUP, one, 0)
        return carry

    lax.fori_loop(0, BLOCKS, forward, 0)

    loads[2].wait()
    taps_ref[8:10, 0 : TAPS - 1] = raw[1].astype(jnp.float32)
    mirror = (
        lax.broadcasted_iota(jnp.int32, (128, 128), 0)
        + lax.broadcasted_iota(jnp.int32, (128, 128), 1)
        == 127
    ).astype(jnp.bfloat16)
    for g in range(TAPS // 128):
        piece = taps_ref[8:16, 128 * g : 128 * g + 128].astype(jnp.bfloat16)
        turned = jnp.dot(piece, mirror, preferred_element_type=jnp.float32)
        taps_ref[2:4, TAPS - 128 * (g + 1) : TAPS - 128 * g] = turned[0:2]
    narrow = lax.broadcasted_iota(jnp.int32, (16, 128), 1) // 32

    def build_source(comp, carry):
        for e in range(8):
            skewed[16 * e : 16 * e + 16, :] = rolled_taps(taps_ref, 2 + comp, e)

        def unit(u, inner):
            for e in range(8):
                at = 256 * (u // 2) + 128 * ((e // 2) % 2) + 64 * lax.rem(u, 2)
                to = pl.ds(pl.multiple_of(at + 32 * (e // 4) + 16 * (e % 2), 16), 16)
                for h in range(2):
                    out = None
                    for i in range(4):
                        back = 2 * (i + h)
                        tile = UNITS - 1 - u + (1 if e < back else 0)
                        row = 16 * ((e - back) % 8)
                        piece = skewed[row : row + 16, pl.ds(pl.multiple_of(tile * 128, 128), 128)]
                        piece = piece.astype(jnp.float32)
                        out = piece if out is None else jnp.where(narrow == i, piece, out)
                    mixed[comp, to, 128 * h : 128 * h + 128] = out.astype(jnp.bfloat16)
            return inner

        lax.fori_loop(0, UNITS, unit, 0)
        return carry

    lax.fori_loop(0, 2, build_source, 0)
    for buffer in (half, half_turned):
        buffer[0 : 2 * SUB, 0:BLOCK] = jnp.zeros((2 * SUB, BLOCK), jnp.bfloat16)
        buffer[2 * SUB : 4 * SUB, WIDTH : WIDTH + BLOCK] = jnp.zeros((2 * SUB, BLOCK), jnp.bfloat16)

    def second(chunk, carry):
        whole(0, send_a, got_a, chunk).wait_recv()

        def turn(g, inner):
            block = jnp.concatenate([got_a[chunk, 4 * g + i] for i in range(4)], axis=0)
            flipped = block.T
            for h in range(2):
                re = flipped[2 * SUB * h : 2 * SUB * h + SUB]
                im = flipped[2 * SUB * h + SUB : 2 * SUB * (h + 1)]
                for top, place in ((0, BLOCK), (2 * SUB, 0)):
                    at = pl.ds(pl.multiple_of(g * BLOCK + place + 128 * h, 128), 128)
                    half[top : top + SUB, at] = re
                    half[top + SUB : top + 2 * SUB, at] = im
                    half_turned[top : top + SUB, at] = -im
                    half_turned[top + SUB : top + 2 * SUB, at] = re
            return inner

        lax.fori_loop(0, PANELS // 4, turn, 0)

        def backward(step, inner):
            shift = (step + 1) // 2
            away = jnp.where(lax.rem(step, 2) == 0, GROUPS // 2 + shift, GROUPS // 2 - shift)
            group = lax.rem(my_group + away, GROUPS)
            at = pl.multiple_of((BLOCKS - 2 - 2 * group) * BLOCK, BLOCK)
            at = pl.ds(at, WIDTH + BLOCK)
            result = jnp.dot(
                half[...], mixed[0, at, :], preferred_element_type=jnp.float32
            ) + jnp.dot(half_turned[...], mixed[1, at, :], preferred_element_type=jnp.float32)
            for b in range(2):
                part = result[2 * SUB * b : 2 * SUB * (b + 1)].astype(jnp.bfloat16)
                rows = jnp.concatenate([part[:, 0:128], part[:, 128:256]], axis=0).T
                for i in range(4):
                    send_b[chunk, group * GROUP + 4 * b + i] = rows[SUB * i : SUB * i + SUB]

            def one(t, inner2):
                post(1, send_b, got_b, chunk, group * GROUP + lax.rem(my_seat + t, GROUP))
                return inner2

            lax.fori_loop(0, GROUP, one, 0)
            return inner

        lax.fori_loop(0, GROUPS, backward, 0)
        return carry

    lax.fori_loop(0, CHUNKS, second, 0)

    def fold(x):
        total = x[0:8]
        for k in range(1, SUB // 8):
            total = total + x[8 * k : 8 * k + 8]
        return total

    def collect(chunk, sums):
        whole(1, send_b, got_b, chunk).wait_recv()

        def tile(g, sums):
            parts = [got_b[chunk, 4 * g + i].astype(jnp.float32) for i in range(4)]
            outs = spread(parts, quarter)
            at = pl.ds(pl.multiple_of(chunk * HALF + g * 128, 128), 128)
            num_re, num_im, energy = sums
            for h in range(2):
                re, im = outs[2 * h], outs[2 * h + 1]
                rows = slice(SUB * h, SUB * h + SUB)
                mult[0, 0, rows, at] = re.astype(jnp.bfloat16)
                mult[0, 1, rows, at] = im.astype(jnp.bfloat16)
                data_re = rec[0, 0, rows, at]
                data_im = rec[0, 1, rows, at]
                num_re = num_re + fold(re * data_re + im * data_im)
                num_im = num_im + fold(re * data_im - im * data_re)
                energy = energy + fold(re * re + im * im)
            return num_re, num_im, energy

        return lax.fori_loop(0, PANELS // 4, tile, sums)

    zero = jnp.zeros((8, 128), jnp.float32)
    sums = lax.fori_loop(0, CHUNKS, collect, (zero, zero, zero))
    column = lax.broadcasted_iota(jnp.int32, (1, 128), 1)
    sums = [jnp.sum(x, keepdims=True) for x in sums]
    mine = jnp.where(column == 0, sums[0], jnp.where(column == 1, sums[1], sums[2]))
    part_out[0:1, 0:1] = mine[None]
    part_in[pl.ds(me, 1), 0:1] = mine[None]

    def share(k, carry):
        target = lax.rem(me + k, PANELS)
        pltpu.make_async_remote_copy(
            src_ref=part_out.at[pl.ds(0, 1), pl.ds(0, 1)],
            dst_ref=part_in.at[pl.ds(me, 1), pl.ds(0, 1)],
            send_sem=send_sem.at[2, 0],
            recv_sem=recv_sem.at[2, 0],
            device_id={"panel": target},
            device_id_type=MESH,
        ).start()
        return carry

    lax.fori_loop(1, PANELS, share, 0)
    for chunk in range(CHUNKS):
        whole(0, send_a, got_a, chunk).wait_send()
        whole(1, send_b, got_b, chunk).wait_send()
    others = pl.ds(0, PANELS - 1)
    shared = pltpu.make_async_remote_copy(
        src_ref=part_in.at[others, pl.ds(0, 1)],
        dst_ref=part_in.at[others, pl.ds(0, 1)],
        send_sem=send_sem.at[2, 0],
        recv_sem=recv_sem.at[2, 0],
        device_id={"panel": lax.rem(me + 1, PANELS)},
        device_id_type=MESH,
    )
    shared.wait_recv()
    total = part_in[0, 0:1]
    for k in range(1, PANELS):
        total = total + part_in[k, 0:1]
    den = total[:, 2:3] + 1e-06
    fit_re = total[:, 0:1] / den
    fit_im = total[:, 1:2] / den

    def subtract(pair, carry):
        at = pl.ds(pl.multiple_of(pair * 128, 128), 128)
        re = mult[0, 0, :, at].astype(jnp.float32)
        im = mult[0, 1, :, at].astype(jnp.float32)
        prim[0, 0, :, at] = rec[0, 0, :, at] - (fit_re * re - fit_im * im)
        prim[0, 1, :, at] = rec[0, 1, :, at] - (fit_re * im + fit_im * re)
        return carry

    lax.fori_loop(0, WIDTH // 128, subtract, 0)
    shared.wait_send()


def per_device(*operands):
    vmem = pltpu.VMEM
    bf16 = jnp.bfloat16
    return pl.pallas_call(
        kernel,
        out_shape=(
            jax.ShapeDtypeStruct((1, 2, ROWS, WIDTH), jnp.float32),
            jax.ShapeDtypeStruct((1, 2, ROWS, WIDTH), bf16),
        ),
        in_specs=[pl.BlockSpec(memory_space=pltpu.HBM)] * 3,
        out_specs=(pl.BlockSpec(memory_space=vmem), pl.BlockSpec(memory_space=vmem)),
        scratch_shapes=[
            vmem((1, 2, ROWS, WIDTH), jnp.float32),
            vmem((2, 2, TAPS - 1), bf16),
            vmem((16, TAPS), jnp.float32),
            vmem((2, 128 * UNITS, BLOCK), bf16),
            vmem((128, TAPS), bf16),
            vmem((2, 128 * UNITS, BLOCK), bf16),
            vmem((2 * ROWS, WIDTH), bf16),
            vmem((2 * ROWS, WIDTH), bf16),
            vmem((4 * SUB, WIDTH + BLOCK), bf16),
            vmem((4 * SUB, WIDTH + BLOCK), bf16),
            vmem((CHUNKS, PANELS, SUB, 128), bf16),
            vmem((CHUNKS, PANELS, SUB, 128), bf16),
            vmem((CHUNKS, PANELS, SUB, 128), bf16),
            vmem((CHUNKS, PANELS, SUB, 128), bf16),
            vmem((1, 8, 128), jnp.float32),
            vmem((PANELS, 8, 128), jnp.float32),
            pltpu.SemaphoreType.DMA((3,)),
            pltpu.SemaphoreType.DMA((3, CHUNKS)),
            pltpu.SemaphoreType.DMA((3, CHUNKS)),
        ],
        compiler_params=pltpu.CompilerParams(
            collective_id=0, has_side_effects=True, vmem_limit_bytes=48 * 1024 * 1024
        ),
    )(*(pltpu.with_memory_space_constraint(x, pltpu.HBM) for x in operands))


def solution(mesh):
    placed = (P("freq", None, "panel", None), P("freq", None, None), P("freq", None, None))
    return jax.shard_map(
        per_device,
        mesh=mesh,
        in_specs=placed,
        out_specs=(P("freq", None, "panel", None), P("freq", None, "panel", None)),
        check_vma=False,
    )
```

```python
import jax
import jax.numpy as jnp
from jax import lax
from jax.experimental import pallas as pl
from jax.experimental.pallas import tpu as pltpu
from jax.sharding import PartitionSpec as P

MESH = pl.DeviceIdType.MESH
PANELS = 32
ROWS = 64
WIDTH = PANELS * ROWS
BLOCK = 256
BLOCKS = WIDTH // BLOCK
TAPS = 2 * WIDTH
UNITS = 2 * (2 * BLOCKS - 1)
CHUNKS = 2
SUB = ROWS // CHUNKS
HALF = WIDTH // 2
GROUP = 8
GROUPS = PANELS // GROUP


def rolled_taps(taps_ref, index, e):
    skew = pltpu.roll(
        jnp.broadcast_to(taps_ref[pl.ds(index, 1), :], (8, TAPS)), 0, 1, stride=1, stride_axis=0
    )
    low = pltpu.roll(skew, 16 * e + TAPS - 128, 1)
    high = pltpu.roll(skew, 16 * e + 8 + TAPS - 128, 1)
    return jnp.concatenate([low, high], axis=0).astype(jnp.bfloat16)


def spread(parts, quarter):
    outs = []
    for i in range(4):
        out = parts[i]
        for k in range(4):
            if k != i:
                out = jnp.where(quarter == k, pltpu.roll(parts[k], 32 * (k - i) % 128, 1), out)
        outs.append(out)
    return outs


def kernel(
    rec_hbm,
    receiver_hbm,
    source_hbm,
    mult,
    rec,
    sums_ref,
    raw,
    taps_ref,
    oper,
    skewed,
    mixed,
    left,
    left_turned,
    half,
    half_turned,
    send_a,
    got_a,
    send_b,
    got_b,
    part_out,
    part_in,
    load_sem,
    send_sem,
    recv_sem,
):
    me = lax.axis_index("panel")
    my_group, my_seat = me // GROUP, lax.rem(me, GROUP)
    barrier = pltpu.get_barrier_semaphore()

    def greet(k, carry):
        pl.semaphore_signal(
            barrier, inc=1, device_id={"panel": lax.rem(me + k, PANELS)}, device_id_type=MESH
        )
        return carry

    loads = [
        pltpu.make_async_copy(receiver_hbm, raw.at[pl.ds(0, 1)], load_sem.at[0]),
        pltpu.make_async_copy(rec_hbm, rec, load_sem.at[1]),
        pltpu.make_async_copy(source_hbm, raw.at[pl.ds(1, 1)], load_sem.at[2]),
    ]
    loads[0].start()
    for comp in range(2):
        for piece in range(ROWS // 8):
            rows = pl.ds(8 * piece, 8)
            pltpu.make_async_copy(
                rec_hbm.at[0, comp, rows], rec.at[0, comp, rows], load_sem.at[1]
            ).start()
    loads[2].start()
    lax.fori_loop(1, PANELS, greet, 0)

    def exchange(stage, src, dst, chunk, target):
        return pltpu.make_async_remote_copy(
            src_ref=src.at[chunk, target],
            dst_ref=dst.at[chunk, me],
            send_sem=send_sem.at[stage, chunk],
            recv_sem=recv_sem.at[stage, chunk, my_group],
            device_id={"panel": target},
            device_id_type=MESH,
        )

    def bulk(stage, src, dst, chunk, group, at, count):
        slots = pl.ds(at, count)
        return pltpu.make_async_remote_copy(
            src_ref=src.at[chunk, slots],
            dst_ref=dst.at[chunk, slots],
            send_sem=send_sem.at[stage, chunk],
            recv_sem=recv_sem.at[stage, chunk, group],
            device_id={"panel": lax.rem(me + 1, PANELS)},
            device_id_type=MESH,
        )

    def sent(stage, src, dst, chunk):
        bulk(stage, src, dst, chunk, 0, 0, PANELS - 1).wait_send()

    def arrived(stage, src, dst, chunk, group):
        @pl.when(group != my_group)
        def _():
            bulk(stage, src, dst, chunk, group, group * GROUP, GROUP).wait_recv()

        @pl.when(group == my_group)
        def _():
            bulk(stage, src, dst, chunk, group, group * GROUP, GROUP - 1).wait_recv()

    def group_of(turn):
        shift = (turn + 1) // 2
        away = jnp.where(lax.rem(turn, 2) == 0, GROUPS // 2 + shift, GROUPS // 2 - shift)
        return lax.rem(my_group + away, GROUPS)

    def post(stage, src, dst, chunk, target):
        @pl.when(target != me)
        def _():
            exchange(stage, src, dst, chunk, target).start()

        @pl.when(target == me)
        def _():
            dst[chunk, me] = src[chunk, me]

    taps_ref[...] = jnp.zeros_like(taps_ref)
    loads[0].wait()
    taps_ref[0:2, 0 : TAPS - 1] = raw[0].astype(jnp.float32)
    taps_ref[0:2, :] = pltpu.roll(taps_ref[0:8, :], 1, 1)[0:2]

    def build_receiver(index, carry):
        for e in range(8):
            rows = rolled_taps(taps_ref, index, e)
            for u in range(UNITS):
                at = 128 * (UNITS - 1 - u)
                oper[index, 128 * u + 16 * e : 128 * u + 16 * e + 16, :] = rows[:, at : at + 256]
        return carry

    lax.fori_loop(0, 2, build_receiver, 0)
    loads[1].wait()
    data_re = rec[0, 0].astype(jnp.bfloat16)
    data_im = rec[0, 1].astype(jnp.bfloat16)
    left[0:ROWS, :] = data_re
    left[ROWS : 2 * ROWS, :] = data_im
    left_turned[0:ROWS, :] = -data_im
    left_turned[ROWS : 2 * ROWS, :] = data_re
    quarter = lax.broadcasted_iota(jnp.int32, (SUB, 128), 1) // 32

    def forward(step, carry):
        chunk = step // GROUPS
        group = group_of(lax.rem(step, GROUPS))
        at = pl.multiple_of((BLOCKS - 1 - chunk * GROUPS - group) * BLOCK, BLOCK)
        result = jnp.dot(
            left[...], oper[0, pl.ds(at, WIDTH), :], preferred_element_type=jnp.float32
        ) + jnp.dot(
            left_turned[...], oper[1, pl.ds(at, WIDTH), :], preferred_element_type=jnp.float32
        )
        for g in range(2):
            lanes = slice(128 * g, 128 * g + 128)
            parts = [
                result[ROWS * comp + SUB * h : ROWS * comp + SUB * h + SUB, lanes]
                for h in range(2)
                for comp in range(2)
            ]
            for i, out in enumerate(spread(parts, quarter)):
                send_a[chunk, group * GROUP + 4 * g + i] = out.astype(jnp.bfloat16)

        @pl.when(step == 0)
        def _():
            pl.semaphore_wait(barrier, PANELS - 1)

        def one(t, inner):
            post(0, send_a, got_a, chunk, group * GROUP + lax.rem(my_seat + t, GROUP))
            return inner

        lax.fori_loop(0, GROUP, one, 0)
        return carry

    lax.fori_loop(0, BLOCKS, forward, 0)

    loads[2].wait()
    taps_ref[8:10, 0 : TAPS - 1] = raw[1].astype(jnp.float32)
    mirror = (
        lax.broadcasted_iota(jnp.int32, (128, 128), 0)
        + lax.broadcasted_iota(jnp.int32, (128, 128), 1)
        == 127
    ).astype(jnp.bfloat16)
    for g in range(TAPS // 128):
        piece = taps_ref[8:16, 128 * g : 128 * g + 128].astype(jnp.bfloat16)
        turned = jnp.dot(piece, mirror, preferred_element_type=jnp.float32)
        taps_ref[2:4, TAPS - 128 * (g + 1) : TAPS - 128 * g] = turned[0:2]
    narrow = lax.broadcasted_iota(jnp.int32, (16, 128), 1) // 32

    def build_source(comp, carry):
        for e in range(8):
            skewed[16 * e : 16 * e + 16, :] = rolled_taps(taps_ref, 2 + comp, e)

        def unit(u, inner):
            for e in range(8):
                at = 256 * (u // 2) + 128 * ((e // 2) % 2) + 64 * lax.rem(u, 2)
                to = pl.ds(pl.multiple_of(at + 32 * (e // 4) + 16 * (e % 2), 16), 16)
                for h in range(2):
                    out = None
                    for i in range(4):
                        back = 2 * (i + h)
                        tile = UNITS - 1 - u + (1 if e < back else 0)
                        row = 16 * ((e - back) % 8)
                        piece = skewed[row : row + 16, pl.ds(pl.multiple_of(tile * 128, 128), 128)]
                        piece = piece.astype(jnp.float32)
                        out = piece if out is None else jnp.where(narrow == i, piece, out)
                    mixed[comp, to, 128 * h : 128 * h + 128] = out.astype(jnp.bfloat16)
            return inner

        lax.fori_loop(0, UNITS, unit, 0)
        return carry

    lax.fori_loop(0, 2, build_source, 0)
    for buffer in (half, half_turned):
        buffer[0 : 2 * SUB, 0:BLOCK] = jnp.zeros((2 * SUB, BLOCK), jnp.bfloat16)
        buffer[2 * SUB : 4 * SUB, WIDTH : WIDTH + BLOCK] = jnp.zeros((2 * SUB, BLOCK), jnp.bfloat16)

    def second(chunk, carry):
        def turn(step, inner):
            group = group_of(step // 2)
            g = 2 * group + lax.rem(step, 2)

            @pl.when(lax.rem(step, 2) == 0)
            def _():
                arrived(0, send_a, got_a, chunk, group)

            block = jnp.concatenate([got_a[chunk, 4 * g + i] for i in range(4)], axis=0)
            flipped = block.T
            for h in range(2):
                re = flipped[2 * SUB * h : 2 * SUB * h + SUB]
                im = flipped[2 * SUB * h + SUB : 2 * SUB * (h + 1)]
                for top, place in ((0, BLOCK), (2 * SUB, 0)):
                    at = pl.ds(pl.multiple_of(g * BLOCK + place + 128 * h, 128), 128)
                    half[top : top + SUB, at] = re
                    half[top + SUB : top + 2 * SUB, at] = im
                    half_turned[top : top + SUB, at] = -im
                    half_turned[top + SUB : top + 2 * SUB, at] = re
            return inner

        lax.fori_loop(0, PANELS // 4, turn, 0)

        def backward(step, inner):
            group = group_of(step)
            at = pl.multiple_of((BLOCKS - 2 - 2 * group) * BLOCK, BLOCK)
            at = pl.ds(at, WIDTH + BLOCK)
            result = jnp.dot(
                half[...], mixed[0, at, :], preferred_element_type=jnp.float32
            ) + jnp.dot(half_turned[...], mixed[1, at, :], preferred_element_type=jnp.float32)
            for b in range(2):
                part = result[2 * SUB * b : 2 * SUB * (b + 1)].astype(jnp.bfloat16)
                rows = jnp.concatenate([part[:, 0:128], part[:, 128:256]], axis=0).T
                for i in range(4):
                    send_b[chunk, group * GROUP + 4 * b + i] = rows[SUB * i : SUB * i + SUB]

            def one(t, inner2):
                post(1, send_b, got_b, chunk, group * GROUP + lax.rem(my_seat + t, GROUP))
                return inner2

            lax.fori_loop(0, GROUP, one, 0)
            return inner

        lax.fori_loop(0, GROUPS, backward, 0)
        return carry

    lax.fori_loop(0, CHUNKS, second, 0)

    def fold(x):
        total = x[0:8]
        for k in range(1, SUB // 8):
            total = total + x[8 * k : 8 * k + 8]
        return total

    def collect(chunk, sums):
        def tile(step, sums):
            group = group_of(step // 2)
            g = 2 * group + lax.rem(step, 2)

            @pl.when(lax.rem(step, 2) == 0)
            def _():
                arrived(1, send_b, got_b, chunk, group)

            parts = [got_b[chunk, 4 * g + i].astype(jnp.float32) for i in range(4)]
            outs = spread(parts, quarter)
            at = pl.ds(pl.multiple_of(chunk * HALF + g * 128, 128), 128)
            num_re, num_im, energy = sums
            for h in range(2):
                re, im = outs[2 * h], outs[2 * h + 1]
                rows = slice(SUB * h, SUB * h + SUB)
                mult[0, 0, rows, at] = re.astype(jnp.bfloat16)
                mult[0, 1, rows, at] = im.astype(jnp.bfloat16)
                data_re = rec[0, 0, rows, at]
                data_im = rec[0, 1, rows, at]
                num_re = num_re + fold(re * data_re + im * data_im)
                num_im = num_im + fold(re * data_im - im * data_re)
                energy = energy + fold(re * re + im * im)
            return num_re, num_im, energy

        return lax.fori_loop(0, PANELS // 4, tile, sums)

    zero = jnp.zeros((8, 128), jnp.float32)
    sums = lax.fori_loop(0, CHUNKS, collect, (zero, zero, zero))
    column = lax.broadcasted_iota(jnp.int32, (1, 128), 1)
    sums = [jnp.sum(x, keepdims=True) for x in sums]
    mine = jnp.where(column == 0, sums[0], jnp.where(column == 1, sums[1], sums[2]))
    part_out[0:1, 0:1] = mine[None]
    part_in[pl.ds(me, 1), 0:1] = mine[None]

    def share(k, carry):
        target = lax.rem(me + k, PANELS)
        pltpu.make_async_remote_copy(
            src_ref=part_out.at[pl.ds(0, 1), pl.ds(0, 1)],
            dst_ref=part_in.at[pl.ds(me, 1), pl.ds(0, 1)],
            send_sem=send_sem.at[2, 0],
            recv_sem=recv_sem.at[2, 0, 0],
            device_id={"panel": target},
            device_id_type=MESH,
        ).start()
        return carry

    lax.fori_loop(1, PANELS, share, 0)
    for chunk in range(CHUNKS):
        sent(0, send_a, got_a, chunk)
        sent(1, send_b, got_b, chunk)
    others = pl.ds(0, PANELS - 1)
    shared = pltpu.make_async_remote_copy(
        src_ref=part_in.at[others, pl.ds(0, 1)],
        dst_ref=part_in.at[others, pl.ds(0, 1)],
        send_sem=send_sem.at[2, 0],
        recv_sem=recv_sem.at[2, 0, 0],
        device_id={"panel": lax.rem(me + 1, PANELS)},
        device_id_type=MESH,
    )
    shared.wait_recv()
    total = part_in[0, 0:1]
    for k in range(1, PANELS):
        total = total + part_in[k, 0:1]
    sums_ref[0:1] = total
    shared.wait_send()


def finish(mult, rec, sums_ref, prim_hbm, mult_hbm, prim, store_sem):
    for comp in range(2):
        for piece in range(ROWS // 16):
            rows = pl.ds(16 * piece, 16)
            pltpu.make_async_copy(
                mult.at[0, comp, rows], mult_hbm.at[0, comp, rows], store_sem.at[0]
            ).start()
    total = sums_ref[0:1]
    den = total[:, 2:3] + 1e-06
    fit_re = jnp.broadcast_to(total[:, 0:1] / den, (16, 256))
    fit_im = jnp.broadcast_to(total[:, 1:2] / den, (16, 256))
    for piece in range(ROWS // 16):
        rows = slice(16 * piece, 16 * piece + 16)
        for pair in range(WIDTH // 256):
            at = slice(256 * pair, 256 * pair + 256)
            re = mult[0, 0, rows, at].astype(jnp.float32)
            im = mult[0, 1, rows, at].astype(jnp.float32)
            prim[0, 0, rows, at] = rec[0, 0, rows, at] - (fit_re * re - fit_im * im)
            prim[0, 1, rows, at] = rec[0, 1, rows, at] - (fit_re * im + fit_im * re)
        for comp in range(2):
            for part in range(2):
                eight = pl.ds(16 * piece + 8 * part, 8)
                pltpu.make_async_copy(
                    prim.at[0, comp, eight], prim_hbm.at[0, comp, eight], store_sem.at[1]
                ).start()
    pltpu.make_async_copy(mult, mult_hbm, store_sem.at[0]).wait()
    pltpu.make_async_copy(prim, prim_hbm, store_sem.at[1]).wait()


def per_device(*operands):
    vmem = pltpu.VMEM
    bf16 = jnp.bfloat16
    outs = (
        jax.ShapeDtypeStruct((1, 2, ROWS, WIDTH), jnp.float32),
        jax.ShapeDtypeStruct((1, 2, ROWS, WIDTH), bf16),
    )
    held = pl.pallas_call(
        kernel,
        out_shape=(outs[1], outs[0], jax.ShapeDtypeStruct((8, 128), jnp.float32)),
        in_specs=[pl.BlockSpec(memory_space=pltpu.HBM)] * 3,
        out_specs=(pl.BlockSpec(memory_space=vmem),) * 3,
        scratch_shapes=[
            vmem((2, 2, TAPS - 1), bf16),
            vmem((16, TAPS), jnp.float32),
            vmem((2, 128 * UNITS, BLOCK), bf16),
            vmem((128, TAPS), bf16),
            vmem((2, 128 * UNITS, BLOCK), bf16),
            vmem((2 * ROWS, WIDTH), bf16),
            vmem((2 * ROWS, WIDTH), bf16),
            vmem((4 * SUB, WIDTH + BLOCK), bf16),
            vmem((4 * SUB, WIDTH + BLOCK), bf16),
            vmem((CHUNKS, PANELS, SUB, 128), bf16),
            vmem((CHUNKS, PANELS, SUB, 128), bf16),
            vmem((CHUNKS, PANELS, SUB, 128), bf16),
            vmem((CHUNKS, PANELS, SUB, 128), bf16),
            vmem((1, 8, 128), jnp.float32),
            vmem((PANELS, 8, 128), jnp.float32),
            pltpu.SemaphoreType.DMA((3,)),
            pltpu.SemaphoreType.DMA((3, CHUNKS)),
            pltpu.SemaphoreType.DMA((3, CHUNKS, GROUPS)),
        ],
        compiler_params=pltpu.CompilerParams(
            collective_id=0, has_side_effects=True, vmem_limit_bytes=48 * 1024 * 1024
        ),
    )(*(pltpu.with_memory_space_constraint(x, pltpu.HBM) for x in operands))
    return pl.pallas_call(
        finish,
        out_shape=outs,
        in_specs=[pl.BlockSpec(memory_space=vmem)] * 3,
        out_specs=(pl.BlockSpec(memory_space=pltpu.HBM),) * 2,
        scratch_shapes=[
            vmem((1, 2, ROWS, WIDTH), jnp.float32),
            pltpu.SemaphoreType.DMA((2,)),
        ],
        compiler_params=pltpu.CompilerParams(vmem_limit_bytes=16 * 1024 * 1024),
    )(*held)


def solution(mesh):
    placed = (P("freq", None, "panel", None), P("freq", None, None), P("freq", None, None))
    return jax.shard_map(
        per_device,
        mesh=mesh,
        in_specs=placed,
        out_specs=(P("freq", None, "panel", None), P("freq", None, "panel", None)),
        check_vma=False,
    )
```

```python
import jax
import jax.numpy as jnp
from jax import lax
from jax.experimental import pallas as pl
from jax.experimental.pallas import tpu as pltpu
from jax.sharding import PartitionSpec as P

MESH = pl.DeviceIdType.MESH
PANELS = 32
ROWS = 64
WIDTH = PANELS * ROWS
BLOCK = 256
BLOCKS = WIDTH // BLOCK
TAPS = 2 * WIDTH
UNITS = 2 * (2 * BLOCKS - 1)
CHUNKS = 2
SUB = ROWS // CHUNKS
HALF = WIDTH // 2
GROUP = 8
GROUPS = PANELS // GROUP


def rolled_taps(taps_ref, index, e):
    skew = pltpu.roll(
        jnp.broadcast_to(taps_ref[pl.ds(index, 1), :], (8, TAPS)), 0, 1, stride=1, stride_axis=0
    )
    low = pltpu.roll(skew, 16 * e + TAPS - 128, 1)
    high = pltpu.roll(skew, 16 * e + 8 + TAPS - 128, 1)
    return jnp.concatenate([low, high], axis=0).astype(jnp.bfloat16)


def spread(parts, quarter):
    outs = []
    for i in range(4):
        out = parts[i]
        for k in range(4):
            if k != i:
                out = jnp.where(quarter == k, pltpu.roll(parts[k], 32 * (k - i) % 128, 1), out)
        outs.append(out)
    return outs


def kernel(
    rec_hbm,
    receiver_hbm,
    source_hbm,
    mult,
    rec,
    sums_ref,
    raw,
    taps_ref,
    oper,
    skewed,
    mixed,
    left,
    left_turned,
    half,
    half_turned,
    send_a,
    got_a,
    send_b,
    got_b,
    part_out,
    part_in,
    load_sem,
    send_sem,
    recv_sem,
):
    me = lax.axis_index("panel")
    my_group, my_seat = me // GROUP, lax.rem(me, GROUP)
    barrier = pltpu.get_barrier_semaphore()

    loads = [
        pltpu.make_async_copy(receiver_hbm, raw.at[pl.ds(0, 1)], load_sem.at[0]),
        pltpu.make_async_copy(rec_hbm, rec, load_sem.at[1]),
        pltpu.make_async_copy(source_hbm, raw.at[pl.ds(1, 1)], load_sem.at[2]),
    ]
    loads[0].start()
    for comp in range(2):
        for piece in range(ROWS // 8):
            rows = pl.ds(8 * piece, 8)
            pltpu.make_async_copy(
                rec_hbm.at[0, comp, rows], rec.at[0, comp, rows], load_sem.at[1]
            ).start()
    loads[2].start()
    for k in range(1, PANELS):
        pl.semaphore_signal(
            barrier, inc=1, device_id={"panel": lax.rem(me + k, PANELS)}, device_id_type=MESH
        )

    def exchange(stage, src, dst, chunk, target):
        return pltpu.make_async_remote_copy(
            src_ref=src.at[chunk, target],
            dst_ref=dst.at[chunk, me],
            send_sem=send_sem.at[stage, chunk],
            recv_sem=recv_sem.at[stage, chunk, my_group],
            device_id={"panel": target},
            device_id_type=MESH,
        )

    def bulk(stage, src, dst, chunk, group, at, count):
        slots = pl.ds(at, count)
        return pltpu.make_async_remote_copy(
            src_ref=src.at[chunk, slots],
            dst_ref=dst.at[chunk, slots],
            send_sem=send_sem.at[stage, chunk],
            recv_sem=recv_sem.at[stage, chunk, group],
            device_id={"panel": lax.rem(me + 1, PANELS)},
            device_id_type=MESH,
        )

    def sent(stage, src, dst, chunk):
        bulk(stage, src, dst, chunk, 0, 0, PANELS - 1).wait_send()

    def arrived(stage, src, dst, chunk, group):
        @pl.when(group != my_group)
        def _():
            bulk(stage, src, dst, chunk, group, group * GROUP, GROUP).wait_recv()

        @pl.when(group == my_group)
        def _():
            bulk(stage, src, dst, chunk, group, group * GROUP, GROUP - 1).wait_recv()

    def group_of(turn):
        away = jnp.where(turn < 2, 2 * turn + 1, 6 - 2 * turn)
        return lax.rem(my_group + away, GROUPS)

    def post(stage, src, dst, chunk, group):
        @pl.when(group != my_group)
        def _():
            exchange(stage, src, dst, chunk, group * GROUP + my_seat).start()

        for t in range(1, GROUP):
            exchange(stage, src, dst, chunk, group * GROUP + lax.rem(my_seat + t, GROUP)).start()

        @pl.when(group == my_group)
        def _():
            dst[chunk, me] = src[chunk, me]

    taps_ref[...] = jnp.zeros_like(taps_ref)
    loads[0].wait()
    taps_ref[0:2, 0 : TAPS - 1] = raw[0].astype(jnp.float32)
    taps_ref[0:2, :] = pltpu.roll(taps_ref[0:8, :], 1, 1)[0:2]

    def build_receiver(index, carry):
        for e in range(8):
            rows = rolled_taps(taps_ref, index, e)
            for u in range(UNITS):
                at = 128 * (UNITS - 1 - u)
                oper[index, 128 * u + 16 * e : 128 * u + 16 * e + 16, :] = rows[:, at : at + 256]
        return carry

    lax.fori_loop(0, 2, build_receiver, 0)
    loads[1].wait()
    data_re = rec[0, 0].astype(jnp.bfloat16)
    data_im = rec[0, 1].astype(jnp.bfloat16)
    left[0:ROWS, :] = data_re
    left[ROWS : 2 * ROWS, :] = data_im
    left_turned[0:ROWS, :] = -data_im
    left_turned[ROWS : 2 * ROWS, :] = data_re
    quarter = lax.broadcasted_iota(jnp.int32, (SUB, 128), 1) // 32

    def forward(step, carry):
        chunk = step // GROUPS
        group = group_of(lax.rem(step, GROUPS))
        at = pl.multiple_of((BLOCKS - 1 - chunk * GROUPS - group) * BLOCK, BLOCK)
        result = jnp.dot(
            left[...], oper[0, pl.ds(at, WIDTH), :], preferred_element_type=jnp.float32
        ) + jnp.dot(
            left_turned[...], oper[1, pl.ds(at, WIDTH), :], preferred_element_type=jnp.float32
        )
        for g in range(2):
            lanes = slice(128 * g, 128 * g + 128)
            parts = [
                result[ROWS * comp + SUB * h : ROWS * comp + SUB * h + SUB, lanes]
                for h in range(2)
                for comp in range(2)
            ]
            for i, out in enumerate(spread(parts, quarter)):
                send_a[chunk, group * GROUP + 4 * g + i] = out.astype(jnp.bfloat16)

        @pl.when(step == 0)
        def _():
            pl.semaphore_wait(barrier, PANELS - 1)

        post(0, send_a, got_a, chunk, group)
        return carry

    lax.fori_loop(0, BLOCKS, forward, 0)

    loads[2].wait()
    taps_ref[8:10, 0 : TAPS - 1] = raw[1].astype(jnp.float32)
    mirror = (
        lax.broadcasted_iota(jnp.int32, (128, 128), 0)
        + lax.broadcasted_iota(jnp.int32, (128, 128), 1)
        == 127
    ).astype(jnp.bfloat16)
    for g in range(TAPS // 128):
        piece = taps_ref[8:16, 128 * g : 128 * g + 128].astype(jnp.bfloat16)
        turned = jnp.dot(piece, mirror, preferred_element_type=jnp.float32)
        taps_ref[2:4, TAPS - 128 * (g + 1) : TAPS - 128 * g] = turned[0:2]
    narrow = lax.broadcasted_iota(jnp.int32, (16, 128), 1) // 32

    def build_source(comp, carry):
        for e in range(8):
            skewed[16 * e : 16 * e + 16, :] = rolled_taps(taps_ref, 2 + comp, e)

        def unit(u, inner):
            for e in range(8):
                at = 256 * (u // 2) + 128 * ((e // 2) % 2) + 64 * lax.rem(u, 2)
                to = pl.ds(pl.multiple_of(at + 32 * (e // 4) + 16 * (e % 2), 16), 16)
                for h in range(2):
                    out = None
                    for i in range(4):
                        back = 2 * (i + h)
                        tile = UNITS - 1 - u + (1 if e < back else 0)
                        row = 16 * ((e - back) % 8)
                        piece = skewed[row : row + 16, pl.ds(pl.multiple_of(tile * 128, 128), 128)]
                        piece = piece.astype(jnp.float32)
                        out = piece if out is None else jnp.where(narrow == i, piece, out)
                    mixed[comp, to, 128 * h : 128 * h + 128] = out.astype(jnp.bfloat16)
            return inner

        lax.fori_loop(0, UNITS, unit, 0)
        return carry

    lax.fori_loop(0, 2, build_source, 0)
    for buffer in (half, half_turned):
        buffer[0 : 2 * SUB, 0:BLOCK] = jnp.zeros((2 * SUB, BLOCK), jnp.bfloat16)
        buffer[2 * SUB : 4 * SUB, WIDTH : WIDTH + BLOCK] = jnp.zeros((2 * SUB, BLOCK), jnp.bfloat16)

    def second(chunk, carry):
        def turn(step, inner):
            group = group_of(step)
            arrived(0, send_a, got_a, chunk, group)
            for part in range(2):
                g = 2 * group + part
                block = jnp.concatenate([got_a[chunk, 4 * g + i] for i in range(4)], axis=0)
                flipped = block.T
                for h in range(2):
                    re = flipped[2 * SUB * h : 2 * SUB * h + SUB]
                    im = flipped[2 * SUB * h + SUB : 2 * SUB * (h + 1)]
                    for top, place in ((0, BLOCK), (2 * SUB, 0)):
                        at = pl.ds(pl.multiple_of(g * BLOCK + place + 128 * h, 128), 128)
                        half[top : top + SUB, at] = re
                        half[top + SUB : top + 2 * SUB, at] = im
                        half_turned[top : top + SUB, at] = -im
                        half_turned[top + SUB : top + 2 * SUB, at] = re
            return inner

        lax.fori_loop(0, GROUPS, turn, 0)

        def backward(step, inner):
            group = group_of(step)
            at = pl.multiple_of((BLOCKS - 2 - 2 * group) * BLOCK, BLOCK)
            at = pl.ds(at, WIDTH + BLOCK)
            result = jnp.dot(
                half[...], mixed[0, at, :], preferred_element_type=jnp.float32
            ) + jnp.dot(half_turned[...], mixed[1, at, :], preferred_element_type=jnp.float32)
            for b in range(2):
                part = result[2 * SUB * b : 2 * SUB * (b + 1)].astype(jnp.bfloat16)
                rows = jnp.concatenate([part[:, 0:128], part[:, 128:256]], axis=0).T
                for i in range(4):
                    send_b[chunk, group * GROUP + 4 * b + i] = rows[SUB * i : SUB * i + SUB]
            post(1, send_b, got_b, chunk, group)
            return inner

        lax.fori_loop(0, GROUPS, backward, 0)
        return carry

    lax.fori_loop(0, CHUNKS, second, 0)

    def fold(x):
        total = x[0:8]
        for k in range(1, SUB // 8):
            total = total + x[8 * k : 8 * k + 8]
        return total

    def collect(chunk, sums):
        def tiles(step, sums):
            group = group_of(step)
            arrived(1, send_b, got_b, chunk, group)
            num_re, num_im, energy = sums
            for part in range(2):
                g = 2 * group + part
                parts = [got_b[chunk, 4 * g + i].astype(jnp.float32) for i in range(4)]
                outs = spread(parts, quarter)
                at = pl.ds(pl.multiple_of(chunk * HALF + g * 128, 128), 128)
                for h in range(2):
                    re, im = outs[2 * h], outs[2 * h + 1]
                    rows = slice(SUB * h, SUB * h + SUB)
                    mult[0, 0, rows, at] = re.astype(jnp.bfloat16)
                    mult[0, 1, rows, at] = im.astype(jnp.bfloat16)
                    data_re = rec[0, 0, rows, at]
                    data_im = rec[0, 1, rows, at]
                    num_re = num_re + fold(re * data_re + im * data_im)
                    num_im = num_im + fold(re * data_im - im * data_re)
                    energy = energy + fold(re * re + im * im)
            return num_re, num_im, energy

        return lax.fori_loop(0, GROUPS, tiles, sums)

    zero = jnp.zeros((8, 128), jnp.float32)
    sums = lax.fori_loop(0, CHUNKS, collect, (zero, zero, zero))
    column = lax.broadcasted_iota(jnp.int32, (1, 128), 1)
    sums = [jnp.sum(x, keepdims=True) for x in sums]
    mine = jnp.where(column == 0, sums[0], jnp.where(column == 1, sums[1], sums[2]))
    part_out[0:1, 0:1] = mine[None]
    part_in[pl.ds(me, 1), 0:1] = mine[None]

    for k in range(1, PANELS):
        target = lax.rem(me + k, PANELS)
        pltpu.make_async_remote_copy(
            src_ref=part_out.at[pl.ds(0, 1), pl.ds(0, 1)],
            dst_ref=part_in.at[pl.ds(me, 1), pl.ds(0, 1)],
            send_sem=send_sem.at[2, 0],
            recv_sem=recv_sem.at[2, 0, 0],
            device_id={"panel": target},
            device_id_type=MESH,
        ).start()
    for chunk in range(CHUNKS):
        sent(0, send_a, got_a, chunk)
        sent(1, send_b, got_b, chunk)
    others = pl.ds(0, PANELS - 1)
    shared = pltpu.make_async_remote_copy(
        src_ref=part_in.at[others, pl.ds(0, 1)],
        dst_ref=part_in.at[others, pl.ds(0, 1)],
        send_sem=send_sem.at[2, 0],
        recv_sem=recv_sem.at[2, 0, 0],
        device_id={"panel": lax.rem(me + 1, PANELS)},
        device_id_type=MESH,
    )
    shared.wait_recv()
    total = part_in[0, 0:1]
    for k in range(1, PANELS):
        total = total + part_in[k, 0:1]
    sums_ref[0:1] = total
    shared.wait_send()


def finish(mult, rec, sums_ref, prim_hbm, mult_hbm, prim, store_sem):
    for comp in range(2):
        for piece in range(ROWS // 16):
            rows = pl.ds(16 * piece, 16)
            pltpu.make_async_copy(
                mult.at[0, comp, rows], mult_hbm.at[0, comp, rows], store_sem.at[0]
            ).start()
    total = sums_ref[0:1]
    den = total[:, 2:3] + 1e-06
    fit_re = jnp.broadcast_to(total[:, 0:1] / den, (16, 256))
    fit_im = jnp.broadcast_to(total[:, 1:2] / den, (16, 256))
    for piece in range(ROWS // 16):
        rows = slice(16 * piece, 16 * piece + 16)
        for pair in range(WIDTH // 256):
            at = slice(256 * pair, 256 * pair + 256)
            re = mult[0, 0, rows, at].astype(jnp.float32)
            im = mult[0, 1, rows, at].astype(jnp.float32)
            prim[0, 0, rows, at] = rec[0, 0, rows, at] - (fit_re * re - fit_im * im)
            prim[0, 1, rows, at] = rec[0, 1, rows, at] - (fit_re * im + fit_im * re)
        for comp in range(2):
            for part in range(2):
                eight = pl.ds(16 * piece + 8 * part, 8)
                pltpu.make_async_copy(
                    prim.at[0, comp, eight], prim_hbm.at[0, comp, eight], store_sem.at[1]
                ).start()
    pltpu.make_async_copy(mult, mult_hbm, store_sem.at[0]).wait()
    pltpu.make_async_copy(prim, prim_hbm, store_sem.at[1]).wait()


def per_device(*operands):
    vmem = pltpu.VMEM
    bf16 = jnp.bfloat16
    outs = (
        jax.ShapeDtypeStruct((1, 2, ROWS, WIDTH), jnp.float32),
        jax.ShapeDtypeStruct((1, 2, ROWS, WIDTH), bf16),
    )
    held = pl.pallas_call(
        kernel,
        out_shape=(outs[1], outs[0], jax.ShapeDtypeStruct((8, 128), jnp.float32)),
        in_specs=[pl.BlockSpec(memory_space=pltpu.HBM)] * 3,
        out_specs=(pl.BlockSpec(memory_space=vmem),) * 3,
        scratch_shapes=[
            vmem((2, 2, TAPS - 1), bf16),
            vmem((16, TAPS), jnp.float32),
            vmem((2, 128 * UNITS, BLOCK), bf16),
            vmem((128, TAPS), bf16),
            vmem((2, 128 * UNITS, BLOCK), bf16),
            vmem((2 * ROWS, WIDTH), bf16),
            vmem((2 * ROWS, WIDTH), bf16),
            vmem((4 * SUB, WIDTH + BLOCK), bf16),
            vmem((4 * SUB, WIDTH + BLOCK), bf16),
            vmem((CHUNKS, PANELS, SUB, 128), bf16),
            vmem((CHUNKS, PANELS, SUB, 128), bf16),
            vmem((CHUNKS, PANELS, SUB, 128), bf16),
            vmem((CHUNKS, PANELS, SUB, 128), bf16),
            vmem((1, 8, 128), jnp.float32),
            vmem((PANELS, 8, 128), jnp.float32),
            pltpu.SemaphoreType.DMA((3,)),
            pltpu.SemaphoreType.DMA((3, CHUNKS)),
            pltpu.SemaphoreType.DMA((3, CHUNKS, GROUPS)),
        ],
        compiler_params=pltpu.CompilerParams(
            collective_id=0, has_side_effects=True, vmem_limit_bytes=48 * 1024 * 1024
        ),
    )(*(pltpu.with_memory_space_constraint(x, pltpu.HBM) for x in operands))
    return pl.pallas_call(
        finish,
        out_shape=outs,
        in_specs=[pl.BlockSpec(memory_space=vmem)] * 3,
        out_specs=(pl.BlockSpec(memory_space=pltpu.HBM),) * 2,
        scratch_shapes=[
            vmem((1, 2, ROWS, WIDTH), jnp.float32),
            pltpu.SemaphoreType.DMA((2,)),
        ],
        compiler_params=pltpu.CompilerParams(vmem_limit_bytes=16 * 1024 * 1024),
    )(*held)


def solution(mesh):
    placed = (P("freq", None, "panel", None), P("freq", None, None), P("freq", None, None))
    return jax.shard_map(
        per_device,
        mesh=mesh,
        in_specs=placed,
        out_specs=(P("freq", None, "panel", None), P("freq", None, "panel", None)),
        check_vma=False,
    )
```

```python
import jax
import jax.numpy as jnp
from jax import lax
from jax.experimental import pallas as pl
from jax.experimental.pallas import tpu as pltpu
from jax.sharding import PartitionSpec as P

MESH = pl.DeviceIdType.MESH
PANELS = 32
ROWS = 64
WIDTH = PANELS * ROWS
BLOCK = 256
BLOCKS = WIDTH // BLOCK
TAPS = 2 * WIDTH
UNITS = 2 * (2 * BLOCKS - 1)
CHUNKS = 2
SUB = ROWS // CHUNKS
HALF = WIDTH // 2
GROUP = 8
GROUPS = PANELS // GROUP


def rolled_taps(taps_ref, index, e):
    skew = pltpu.roll(
        jnp.broadcast_to(taps_ref[pl.ds(index, 1), :], (8, TAPS)), 0, 1, stride=1, stride_axis=0
    )
    low = pltpu.roll(skew, 16 * e + TAPS - 128, 1)
    high = pltpu.roll(skew, 16 * e + 8 + TAPS - 128, 1)
    return jnp.concatenate([low, high], axis=0).astype(jnp.bfloat16)


def spread(parts, quarter):
    outs = []
    for i in range(4):
        out = parts[i]
        for k in range(4):
            if k != i:
                out = jnp.where(quarter == k, pltpu.roll(parts[k], 32 * (k - i) % 128, 1), out)
        outs.append(out)
    return outs


def kernel(
    rec_hbm,
    receiver_hbm,
    source_hbm,
    mult,
    rec,
    sums_ref,
    raw,
    taps_ref,
    oper,
    skewed,
    mixed,
    left,
    left_turned,
    half,
    half_turned,
    send_a,
    got_a,
    send_b,
    got_b,
    part_out,
    part_in,
    load_sem,
    send_sem,
    recv_sem,
):
    me = lax.axis_index("panel")
    my_group, my_seat = me // GROUP, lax.rem(me, GROUP)
    barrier = pltpu.get_barrier_semaphore()

    loads = [
        pltpu.make_async_copy(receiver_hbm, raw.at[pl.ds(0, 1)], load_sem.at[0]),
        pltpu.make_async_copy(rec_hbm, rec, load_sem.at[1]),
        pltpu.make_async_copy(source_hbm, raw.at[pl.ds(1, 1)], load_sem.at[2]),
    ]
    loads[0].start()
    for comp in range(2):
        for piece in range(ROWS // 8):
            rows = pl.ds(8 * piece, 8)
            pltpu.make_async_copy(
                rec_hbm.at[0, comp, rows], rec.at[0, comp, rows], load_sem.at[1]
            ).start()
    loads[2].start()
    for k in range(1, PANELS):
        pl.semaphore_signal(
            barrier, inc=1, device_id={"panel": lax.rem(me + k, PANELS)}, device_id_type=MESH
        )

    def exchange(stage, src, dst, chunk, target):
        return pltpu.make_async_remote_copy(
            src_ref=src.at[chunk, target],
            dst_ref=dst.at[chunk, me],
            send_sem=send_sem.at[stage, chunk],
            recv_sem=recv_sem.at[stage, chunk, my_group],
            device_id={"panel": target},
            device_id_type=MESH,
        )

    def bulk(stage, src, dst, chunk, group, at, count):
        slots = pl.ds(at, count)
        return pltpu.make_async_remote_copy(
            src_ref=src.at[chunk, slots],
            dst_ref=dst.at[chunk, slots],
            send_sem=send_sem.at[stage, chunk],
            recv_sem=recv_sem.at[stage, chunk, group],
            device_id={"panel": lax.rem(me + 1, PANELS)},
            device_id_type=MESH,
        )

    def sent(stage, src, dst, chunk):
        bulk(stage, src, dst, chunk, 0, 0, PANELS - 1).wait_send()

    def arrived(stage, src, dst, chunk, group):
        @pl.when(group != my_group)
        def _():
            bulk(stage, src, dst, chunk, group, group * GROUP, GROUP).wait_recv()

        @pl.when(group == my_group)
        def _():
            bulk(stage, src, dst, chunk, group, group * GROUP, GROUP - 1).wait_recv()

    def group_of(turn):
        away = jnp.where(turn < 2, 2 * turn + 1, 2 * turn - 4)
        return lax.rem(my_group + away, GROUPS)

    def post(stage, src, dst, chunk, group):
        @pl.when(group != my_group)
        def _():
            exchange(stage, src, dst, chunk, group * GROUP + my_seat).start()

        for t in range(1, GROUP):
            exchange(stage, src, dst, chunk, group * GROUP + lax.rem(my_seat + t, GROUP)).start()

        @pl.when(group == my_group)
        def _():
            dst[chunk, me] = src[chunk, me]

    taps_ref[...] = jnp.zeros_like(taps_ref)
    loads[0].wait()
    taps_ref[0:2, 0 : TAPS - 1] = raw[0].astype(jnp.float32)
    taps_ref[0:2, :] = pltpu.roll(taps_ref[0:8, :], 1, 1)[0:2]

    def build_receiver(index, carry):
        for e in range(8):
            rows = rolled_taps(taps_ref, index, e)
            for u in range(UNITS + 1):
                at = 128 * (UNITS - u)
                oper[index, 128 * u + 16 * e : 128 * u + 16 * e + 16, :] = rows[:, at : at + 128]
        return carry

    lax.fori_loop(0, 2, build_receiver, 0)
    loads[1].wait()
    data_re = rec[0, 0].astype(jnp.bfloat16)
    data_im = rec[0, 1].astype(jnp.bfloat16)
    left[0:ROWS, :] = data_re
    left[ROWS : 2 * ROWS, :] = data_im
    left_turned[0:ROWS, :] = -data_im
    left_turned[ROWS : 2 * ROWS, :] = data_re
    quarter = lax.broadcasted_iota(jnp.int32, (SUB, 128), 1) // 32

    def forward(step, carry):
        chunk = step // GROUPS
        group = group_of(lax.rem(step, GROUPS))
        at = pl.multiple_of((BLOCKS - 1 - chunk * GROUPS - group) * BLOCK, BLOCK)
        terms = []
        for index, lhs in enumerate((left, left_turned)):
            halves = [oper[index, pl.ds(at + 128, WIDTH), :], oper[index, pl.ds(at, WIDTH), :]]
            rhs = jnp.concatenate(halves, axis=1)
            terms.append(jnp.dot(lhs[...], rhs, preferred_element_type=jnp.float32))
        result = terms[0] + terms[1]
        for g in range(2):
            lanes = slice(128 * g, 128 * g + 128)
            parts = [
                result[ROWS * comp + SUB * h : ROWS * comp + SUB * h + SUB, lanes]
                for h in range(2)
                for comp in range(2)
            ]
            for i, out in enumerate(spread(parts, quarter)):
                send_a[chunk, group * GROUP + 4 * g + i] = out.astype(jnp.bfloat16)

        @pl.when(step == 0)
        def _():
            pl.semaphore_wait(barrier, PANELS - 1)

        post(0, send_a, got_a, chunk, group)
        return carry

    lax.fori_loop(0, BLOCKS, forward, 0)

    loads[2].wait()
    taps_ref[8:10, 0 : TAPS - 1] = raw[1].astype(jnp.float32)
    mirror = (
        lax.broadcasted_iota(jnp.int32, (128, 128), 0)
        + lax.broadcasted_iota(jnp.int32, (128, 128), 1)
        == 127
    ).astype(jnp.bfloat16)
    for g in range(TAPS // 128):
        piece = taps_ref[8:16, 128 * g : 128 * g + 128].astype(jnp.bfloat16)
        turned = jnp.dot(piece, mirror, preferred_element_type=jnp.float32)
        taps_ref[2:4, TAPS - 128 * (g + 1) : TAPS - 128 * g] = turned[0:2]
    narrow = lax.broadcasted_iota(jnp.int32, (16, 128), 1) // 32

    def build_source(comp, carry):
        for e in range(8):
            skewed[16 * e : 16 * e + 16, :] = rolled_taps(taps_ref, 2 + comp, e)

        def unit(u, inner):
            for e in range(8):
                at = 256 * (u // 2) + 128 * ((e // 2) % 2) + 64 * lax.rem(u, 2)
                to = pl.ds(pl.multiple_of(at + 32 * (e // 4) + 16 * (e % 2), 16), 16)
                for h in range(2):
                    out = None
                    for i in range(4):
                        back = 2 * (i + h)
                        tile = UNITS - 1 - u + (1 if e < back else 0)
                        row = 16 * ((e - back) % 8)
                        piece = skewed[row : row + 16, pl.ds(pl.multiple_of(tile * 128, 128), 128)]
                        piece = piece.astype(jnp.float32)
                        out = piece if out is None else jnp.where(narrow == i, piece, out)
                    mixed[comp, to, 128 * h : 128 * h + 128] = out.astype(jnp.bfloat16)
            return inner

        lax.fori_loop(0, UNITS, unit, 0)
        return carry

    lax.fori_loop(0, 2, build_source, 0)
    for buffer in (half, half_turned):
        buffer[0 : 2 * SUB, 0:BLOCK] = jnp.zeros((2 * SUB, BLOCK), jnp.bfloat16)
        buffer[2 * SUB : 4 * SUB, WIDTH : WIDTH + BLOCK] = jnp.zeros((2 * SUB, BLOCK), jnp.bfloat16)

    def second(chunk, carry):
        def turn(step, inner):
            group = group_of(step)
            arrived(0, send_a, got_a, chunk, group)
            for part in range(2):
                g = 2 * group + part
                block = jnp.concatenate([got_a[chunk, 4 * g + i] for i in range(4)], axis=0)
                flipped = block.T
                for h in range(2):
                    re = flipped[2 * SUB * h : 2 * SUB * h + SUB]
                    im = flipped[2 * SUB * h + SUB : 2 * SUB * (h + 1)]
                    for top, place in ((0, BLOCK), (2 * SUB, 0)):
                        at = pl.ds(pl.multiple_of(g * BLOCK + place + 128 * h, 128), 128)
                        half[top : top + SUB, at] = re
                        half[top + SUB : top + 2 * SUB, at] = im
                        half_turned[top : top + SUB, at] = -im
                        half_turned[top + SUB : top + 2 * SUB, at] = re
            return inner

        lax.fori_loop(0, GROUPS, turn, 0)

        def backward(step, inner):
            group = group_of(step)
            at = pl.multiple_of((BLOCKS - 2 - 2 * group) * BLOCK, BLOCK)
            at = pl.ds(at, WIDTH + BLOCK)
            result = jnp.dot(
                half[...], mixed[0, at, :], preferred_element_type=jnp.float32
            ) + jnp.dot(half_turned[...], mixed[1, at, :], preferred_element_type=jnp.float32)
            for b in range(2):
                part = result[2 * SUB * b : 2 * SUB * (b + 1)].astype(jnp.bfloat16)
                rows = jnp.concatenate([part[:, 0:128], part[:, 128:256]], axis=0).T
                for i in range(4):
                    send_b[chunk, group * GROUP + 4 * b + i] = rows[SUB * i : SUB * i + SUB]
            post(1, send_b, got_b, chunk, group)
            return inner

        lax.fori_loop(0, GROUPS, backward, 0)
        return carry

    lax.fori_loop(0, CHUNKS, second, 0)

    def fold(x):
        total = x[0:8]
        for k in range(1, SUB // 8):
            total = total + x[8 * k : 8 * k + 8]
        return total

    def collect(chunk, sums):
        def tiles(step, sums):
            group = group_of(step)
            arrived(1, send_b, got_b, chunk, group)
            num_re, num_im, energy = sums
            for part in range(2):
                g = 2 * group + part
                parts = [got_b[chunk, 4 * g + i].astype(jnp.float32) for i in range(4)]
                outs = spread(parts, quarter)
                at = pl.ds(pl.multiple_of(chunk * HALF + g * 128, 128), 128)
                for h in range(2):
                    re, im = outs[2 * h], outs[2 * h + 1]
                    rows = slice(SUB * h, SUB * h + SUB)
                    mult[0, 0, rows, at] = re.astype(jnp.bfloat16)
                    mult[0, 1, rows, at] = im.astype(jnp.bfloat16)
                    data_re = rec[0, 0, rows, at]
                    data_im = rec[0, 1, rows, at]
                    num_re = num_re + fold(re * data_re + im * data_im)
                    num_im = num_im + fold(re * data_im - im * data_re)
                    energy = energy + fold(re * re + im * im)
            return num_re, num_im, energy

        return lax.fori_loop(0, GROUPS, tiles, sums)

    zero = jnp.zeros((8, 128), jnp.float32)
    sums = lax.fori_loop(0, CHUNKS, collect, (zero, zero, zero))
    column = lax.broadcasted_iota(jnp.int32, (1, 128), 1)
    sums = [jnp.sum(x, keepdims=True) for x in sums]
    mine = jnp.where(column == 0, sums[0], jnp.where(column == 1, sums[1], sums[2]))
    part_out[0:1, 0:1] = mine[None]
    part_in[pl.ds(me, 1), 0:1] = mine[None]

    for k in range(1, PANELS):
        target = lax.rem(me + k, PANELS)
        pltpu.make_async_remote_copy(
            src_ref=part_out.at[pl.ds(0, 1), pl.ds(0, 1)],
            dst_ref=part_in.at[pl.ds(me, 1), pl.ds(0, 1)],
            send_sem=send_sem.at[2, 0],
            recv_sem=recv_sem.at[2, 0, 0],
            device_id={"panel": target},
            device_id_type=MESH,
        ).start()
    for chunk in range(CHUNKS):
        sent(0, send_a, got_a, chunk)
        sent(1, send_b, got_b, chunk)
    others = pl.ds(0, PANELS - 1)
    shared = pltpu.make_async_remote_copy(
        src_ref=part_in.at[others, pl.ds(0, 1)],
        dst_ref=part_in.at[others, pl.ds(0, 1)],
        send_sem=send_sem.at[2, 0],
        recv_sem=recv_sem.at[2, 0, 0],
        device_id={"panel": lax.rem(me + 1, PANELS)},
        device_id_type=MESH,
    )
    shared.wait_recv()
    total = part_in[0, 0:1]
    for k in range(1, PANELS):
        total = total + part_in[k, 0:1]
    sums_ref[0:1] = total
    shared.wait_send()


def finish(mult, rec, sums_ref, prim_hbm, mult_hbm, prim, store_sem):
    for comp in range(2):
        for piece in range(ROWS // 16):
            rows = pl.ds(16 * piece, 16)
            pltpu.make_async_copy(
                mult.at[0, comp, rows], mult_hbm.at[0, comp, rows], store_sem.at[0]
            ).start()
    total = sums_ref[0:1]
    den = total[:, 2:3] + 1e-06
    fit_re = jnp.broadcast_to(total[:, 0:1] / den, (16, 256))
    fit_im = jnp.broadcast_to(total[:, 1:2] / den, (16, 256))
    for piece in range(ROWS // 16):
        rows = slice(16 * piece, 16 * piece + 16)
        for pair in range(WIDTH // 256):
            at = slice(256 * pair, 256 * pair + 256)
            re = mult[0, 0, rows, at].astype(jnp.float32)
            im = mult[0, 1, rows, at].astype(jnp.float32)
            prim[0, 0, rows, at] = rec[0, 0, rows, at] - (fit_re * re - fit_im * im)
            prim[0, 1, rows, at] = rec[0, 1, rows, at] - (fit_re * im + fit_im * re)
        for comp in range(2):
            for part in range(2):
                eight = pl.ds(16 * piece + 8 * part, 8)
                pltpu.make_async_copy(
                    prim.at[0, comp, eight], prim_hbm.at[0, comp, eight], store_sem.at[1]
                ).start()
    pltpu.make_async_copy(mult, mult_hbm, store_sem.at[0]).wait()
    pltpu.make_async_copy(prim, prim_hbm, store_sem.at[1]).wait()


def per_device(*operands):
    vmem = pltpu.VMEM
    bf16 = jnp.bfloat16
    outs = (
        jax.ShapeDtypeStruct((1, 2, ROWS, WIDTH), jnp.float32),
        jax.ShapeDtypeStruct((1, 2, ROWS, WIDTH), bf16),
    )
    held = pl.pallas_call(
        kernel,
        out_shape=(outs[1], outs[0], jax.ShapeDtypeStruct((8, 128), jnp.float32)),
        in_specs=[pl.BlockSpec(memory_space=pltpu.HBM)] * 3,
        out_specs=(pl.BlockSpec(memory_space=vmem),) * 3,
        scratch_shapes=[
            vmem((2, 2, TAPS - 1), bf16),
            vmem((16, TAPS), jnp.float32),
            vmem((2, 128 * (UNITS + 1), 128), bf16),
            vmem((128, TAPS), bf16),
            vmem((2, 128 * UNITS, BLOCK), bf16),
            vmem((2 * ROWS, WIDTH), bf16),
            vmem((2 * ROWS, WIDTH), bf16),
            vmem((4 * SUB, WIDTH + BLOCK), bf16),
            vmem((4 * SUB, WIDTH + BLOCK), bf16),
            vmem((CHUNKS, PANELS, SUB, 128), bf16),
            vmem((CHUNKS, PANELS, SUB, 128), bf16),
            vmem((CHUNKS, PANELS, SUB, 128), bf16),
            vmem((CHUNKS, PANELS, SUB, 128), bf16),
            vmem((1, 8, 128), jnp.float32),
            vmem((PANELS, 8, 128), jnp.float32),
            pltpu.SemaphoreType.DMA((3,)),
            pltpu.SemaphoreType.DMA((3, CHUNKS)),
            pltpu.SemaphoreType.DMA((3, CHUNKS, GROUPS)),
        ],
        compiler_params=pltpu.CompilerParams(
            collective_id=0, has_side_effects=True, vmem_limit_bytes=48 * 1024 * 1024
        ),
    )(*(pltpu.with_memory_space_constraint(x, pltpu.HBM) for x in operands))
    return pl.pallas_call(
        finish,
        out_shape=outs,
        in_specs=[pl.BlockSpec(memory_space=vmem)] * 3,
        out_specs=(pl.BlockSpec(memory_space=pltpu.HBM),) * 2,
        scratch_shapes=[
            vmem((1, 2, ROWS, WIDTH), jnp.float32),
            pltpu.SemaphoreType.DMA((2,)),
        ],
        compiler_params=pltpu.CompilerParams(vmem_limit_bytes=16 * 1024 * 1024),
    )(*held)


def solution(mesh):
    placed = (P("freq", None, "panel", None), P("freq", None, None), P("freq", None, None))
    return jax.shard_map(
        per_device,
        mesh=mesh,
        in_specs=placed,
        out_specs=(P("freq", None, "panel", None), P("freq", None, "panel", None)),
        check_vma=False,
    )
```

```python
import jax
import jax.numpy as jnp
from jax import lax
from jax.experimental import pallas as pl
from jax.experimental.pallas import tpu as pltpu
from jax.sharding import PartitionSpec as P

MESH = pl.DeviceIdType.MESH
PANELS = 32
ROWS = 64
WIDTH = PANELS * ROWS
BLOCK = 256
BLOCKS = WIDTH // BLOCK
TAPS = 2 * WIDTH
UNITS = 2 * (2 * BLOCKS - 1)
CHUNKS = 2
SUB = ROWS // CHUNKS
HALF = WIDTH // 2
GROUP = 8
GROUPS = PANELS // GROUP


def rolled_taps(taps_ref, index, e):
    skew = pltpu.roll(
        jnp.broadcast_to(taps_ref[pl.ds(index, 1), :], (8, TAPS)), 0, 1, stride=1, stride_axis=0
    )
    low = pltpu.roll(skew, 16 * e + TAPS - 128, 1)
    high = pltpu.roll(skew, 16 * e + 8 + TAPS - 128, 1)
    return jnp.concatenate([low, high], axis=0).astype(jnp.bfloat16)


def spread(parts, quarter):
    outs = []
    for i in range(4):
        out = parts[i]
        for k in range(4):
            if k != i:
                out = jnp.where(quarter == k, pltpu.roll(parts[k], 32 * (k - i) % 128, 1), out)
        outs.append(out)
    return outs


def kernel(
    rec_hbm,
    receiver_hbm,
    source_hbm,
    mult,
    rec,
    sums_ref,
    raw,
    taps_ref,
    oper,
    skewed,
    mixed,
    left,
    left_turned,
    half,
    half_turned,
    send_a,
    got_a,
    send_b,
    got_b,
    part_out,
    part_in,
    load_sem,
    send_sem,
    recv_sem,
):
    me = lax.axis_index("panel")
    my_group, my_seat = me // GROUP, lax.rem(me, GROUP)
    barrier = pltpu.get_barrier_semaphore()

    loads = [
        pltpu.make_async_copy(receiver_hbm, raw.at[pl.ds(0, 1)], load_sem.at[0]),
        pltpu.make_async_copy(rec_hbm, rec, load_sem.at[1]),
        pltpu.make_async_copy(source_hbm, raw.at[pl.ds(1, 1)], load_sem.at[2]),
    ]
    loads[0].start()
    for comp in range(2):
        for piece in range(ROWS // 8):
            rows = pl.ds(8 * piece, 8)
            pltpu.make_async_copy(
                rec_hbm.at[0, comp, rows], rec.at[0, comp, rows], load_sem.at[1]
            ).start()
    loads[2].start()
    for k in range(1, PANELS):
        pl.semaphore_signal(
            barrier, inc=1, device_id={"panel": lax.rem(me + k, PANELS)}, device_id_type=MESH
        )

    def exchange(stage, src, dst, chunk, target):
        return pltpu.make_async_remote_copy(
            src_ref=src.at[chunk, target],
            dst_ref=dst.at[chunk, me],
            send_sem=send_sem.at[stage, chunk],
            recv_sem=recv_sem.at[stage, chunk, my_group],
            device_id={"panel": target},
            device_id_type=MESH,
        )

    def bulk(stage, src, dst, chunk, group, at, count):
        slots = pl.ds(at, count)
        return pltpu.make_async_remote_copy(
            src_ref=src.at[chunk, slots],
            dst_ref=dst.at[chunk, slots],
            send_sem=send_sem.at[stage, chunk],
            recv_sem=recv_sem.at[stage, chunk, group],
            device_id={"panel": lax.rem(me + 1, PANELS)},
            device_id_type=MESH,
        )

    def sent(stage, src, dst, chunk):
        bulk(stage, src, dst, chunk, 0, 0, PANELS - 1).wait_send()

    def arrived(stage, src, dst, chunk, group):
        @pl.when(group != my_group)
        def _():
            bulk(stage, src, dst, chunk, group, group * GROUP, GROUP).wait_recv()

        @pl.when(group == my_group)
        def _():
            bulk(stage, src, dst, chunk, group, group * GROUP, GROUP - 1).wait_recv()

    def group_of(turn):
        away = jnp.where(turn < 2, 2 * turn + 1, 6 - 2 * turn)
        return lax.rem(my_group + away, GROUPS)

    def post(stage, src, dst, chunk, group):
        @pl.when(group != my_group)
        def _():
            exchange(stage, src, dst, chunk, group * GROUP + my_seat).start()

        for t in range(1, GROUP):
            exchange(stage, src, dst, chunk, group * GROUP + lax.rem(my_seat + t, GROUP)).start()

        @pl.when(group == my_group)
        def _():
            dst[chunk, me] = src[chunk, me]

    taps_ref[...] = jnp.zeros_like(taps_ref)
    loads[0].wait()
    taps_ref[0:2, 0 : TAPS - 1] = raw[0].astype(jnp.float32)
    taps_ref[0:2, :] = pltpu.roll(taps_ref[0:8, :], 1, 1)[0:2]

    def build_receiver(index, carry):
        for e in range(8):
            rows = rolled_taps(taps_ref, index, e)
            for u in range(UNITS + 1):
                at = 128 * (UNITS - u)
                oper[index, 128 * u + 16 * e : 128 * u + 16 * e + 16, :] = rows[:, at : at + 128]
        return carry

    lax.fori_loop(0, 2, build_receiver, 0)
    loads[1].wait()
    data_re = rec[0, 0].astype(jnp.bfloat16)
    data_im = rec[0, 1].astype(jnp.bfloat16)
    left[0:ROWS, :] = data_re
    left[ROWS : 2 * ROWS, :] = data_im
    left_turned[0:ROWS, :] = -data_im
    left_turned[ROWS : 2 * ROWS, :] = data_re
    quarter = lax.broadcasted_iota(jnp.int32, (SUB, 128), 1) // 32

    def forward(step, carry):
        chunk = step // GROUPS
        group = group_of(lax.rem(step, GROUPS))
        at = pl.multiple_of((BLOCKS - 1 - chunk * GROUPS - group) * BLOCK, BLOCK)
        terms = []
        for index, lhs in enumerate((left, left_turned)):
            halves = [oper[index, pl.ds(at + 128, WIDTH), :], oper[index, pl.ds(at, WIDTH), :]]
            rhs = jnp.concatenate(halves, axis=1)
            terms.append(jnp.dot(lhs[...], rhs, preferred_element_type=jnp.float32))
        result = terms[0] + terms[1]
        for g in range(2):
            lanes = slice(128 * g, 128 * g + 128)
            parts = [
                result[ROWS * comp + SUB * h : ROWS * comp + SUB * h + SUB, lanes]
                for h in range(2)
                for comp in range(2)
            ]
            for i, out in enumerate(spread(parts, quarter)):
                send_a[chunk, group * GROUP + 4 * g + i] = out.astype(jnp.bfloat16)

        @pl.when(step == 0)
        def _():
            pl.semaphore_wait(barrier, PANELS - 1)

        post(0, send_a, got_a, chunk, group)
        return carry

    lax.fori_loop(0, BLOCKS, forward, 0)

    loads[2].wait()
    taps_ref[8:10, 0 : TAPS - 1] = raw[1].astype(jnp.float32)
    mirror = (
        lax.broadcasted_iota(jnp.int32, (128, 128), 0)
        + lax.broadcasted_iota(jnp.int32, (128, 128), 1)
        == 127
    ).astype(jnp.bfloat16)
    for g in range(TAPS // 128):
        piece = taps_ref[8:16, 128 * g : 128 * g + 128].astype(jnp.bfloat16)
        turned = jnp.dot(piece, mirror, preferred_element_type=jnp.float32)
        taps_ref[2:4, TAPS - 128 * (g + 1) : TAPS - 128 * g] = turned[0:2]
    narrow = lax.broadcasted_iota(jnp.int32, (16, 128), 1) // 32

    def build_source(comp, carry):
        for e in range(8):
            skewed[16 * e : 16 * e + 16, :] = rolled_taps(taps_ref, 2 + comp, e)

        def unit(u, inner):
            for e in range(8):
                at = 256 * (u // 2) + 128 * ((e // 2) % 2) + 64 * lax.rem(u, 2)
                to = pl.ds(pl.multiple_of(at + 32 * (e // 4) + 16 * (e % 2), 16), 16)
                for h in range(2):
                    out = None
                    for i in range(4):
                        back = 2 * (i + h)
                        tile = UNITS - 1 - u + (1 if e < back else 0)
                        row = 16 * ((e - back) % 8)
                        piece = skewed[row : row + 16, pl.ds(pl.multiple_of(tile * 128, 128), 128)]
                        piece = piece.astype(jnp.float32)
                        out = piece if out is None else jnp.where(narrow == i, piece, out)
                    mixed[comp, to, 128 * h : 128 * h + 128] = out.astype(jnp.bfloat16)
            return inner

        lax.fori_loop(0, UNITS, unit, 0)
        return carry

    lax.fori_loop(0, 2, build_source, 0)
    for buffer in (half, half_turned):
        buffer[0 : 2 * SUB, 0:BLOCK] = jnp.zeros((2 * SUB, BLOCK), jnp.bfloat16)
        buffer[2 * SUB : 4 * SUB, WIDTH : WIDTH + BLOCK] = jnp.zeros((2 * SUB, BLOCK), jnp.bfloat16)

    def second(chunk, carry):
        def turn(step, inner):
            group = group_of(step)
            arrived(0, send_a, got_a, chunk, group)
            for part in range(2):
                g = 2 * group + part
                block = jnp.concatenate([got_a[chunk, 4 * g + i] for i in range(4)], axis=0)
                flipped = block.T
                for h in range(2):
                    re = flipped[2 * SUB * h : 2 * SUB * h + SUB]
                    im = flipped[2 * SUB * h + SUB : 2 * SUB * (h + 1)]
                    for top, place in ((0, BLOCK), (2 * SUB, 0)):
                        at = pl.ds(pl.multiple_of(g * BLOCK + place + 128 * h, 128), 128)
                        half[top : top + SUB, at] = re
                        half[top + SUB : top + 2 * SUB, at] = im
                        half_turned[top : top + SUB, at] = -im
                        half_turned[top + SUB : top + 2 * SUB, at] = re
            return inner

        lax.fori_loop(0, GROUPS, turn, 0)

        def backward(step, inner):
            group = group_of(step)
            at = pl.multiple_of((BLOCKS - 2 - 2 * group) * BLOCK, BLOCK)
            at = pl.ds(at, WIDTH + BLOCK)
            result = jnp.dot(
                half[...], mixed[0, at, :], preferred_element_type=jnp.float32
            ) + jnp.dot(half_turned[...], mixed[1, at, :], preferred_element_type=jnp.float32)
            for b in range(2):
                part = result[2 * SUB * b : 2 * SUB * (b + 1)].astype(jnp.bfloat16)
                rows = jnp.concatenate([part[:, 0:128], part[:, 128:256]], axis=0).T
                for i in range(4):
                    send_b[chunk, group * GROUP + 4 * b + i] = rows[SUB * i : SUB * i + SUB]
            post(1, send_b, got_b, chunk, group)
            return inner

        lax.fori_loop(0, GROUPS, backward, 0)
        return carry

    lax.fori_loop(0, CHUNKS, second, 0)

    def fold(x):
        total = x[0:8]
        for k in range(1, SUB // 8):
            total = total + x[8 * k : 8 * k + 8]
        return total

    def collect(chunk, sums):
        def tiles(step, sums):
            group = group_of(step)
            arrived(1, send_b, got_b, chunk, group)
            num_re, num_im, energy = sums
            for part in range(2):
                g = 2 * group + part
                parts = [got_b[chunk, 4 * g + i].astype(jnp.float32) for i in range(4)]
                outs = spread(parts, quarter)
                at = pl.ds(pl.multiple_of(chunk * HALF + g * 128, 128), 128)
                for h in range(2):
                    re, im = outs[2 * h], outs[2 * h + 1]
                    rows = slice(SUB * h, SUB * h + SUB)
                    mult[0, 0, rows, at] = re.astype(jnp.bfloat16)
                    mult[0, 1, rows, at] = im.astype(jnp.bfloat16)
                    data_re = rec[0, 0, rows, at]
                    data_im = rec[0, 1, rows, at]
                    num_re = num_re + fold(re * data_re + im * data_im)
                    num_im = num_im + fold(re * data_im - im * data_re)
                    energy = energy + fold(re * re + im * im)
            return num_re, num_im, energy

        return lax.fori_loop(0, GROUPS, tiles, sums)

    zero = jnp.zeros((8, 128), jnp.float32)
    sums = lax.fori_loop(0, CHUNKS, collect, (zero, zero, zero))
    column = lax.broadcasted_iota(jnp.int32, (1, 128), 1)
    sums = [jnp.sum(x, keepdims=True) for x in sums]
    mine = jnp.where(column == 0, sums[0], jnp.where(column == 1, sums[1], sums[2]))
    part_out[0:1, 0:1] = mine[None]
    part_in[pl.ds(me, 1), 0:1] = mine[None]

    for k in range(1, PANELS):
        target = lax.rem(me + k, PANELS)
        pltpu.make_async_remote_copy(
            src_ref=part_out.at[pl.ds(0, 1), pl.ds(0, 1)],
            dst_ref=part_in.at[pl.ds(me, 1), pl.ds(0, 1)],
            send_sem=send_sem.at[2, 0],
            recv_sem=recv_sem.at[2, 0, 0],
            device_id={"panel": target},
            device_id_type=MESH,
        ).start()
    for chunk in range(CHUNKS):
        sent(0, send_a, got_a, chunk)
        sent(1, send_b, got_b, chunk)
    others = pl.ds(0, PANELS - 1)
    shared = pltpu.make_async_remote_copy(
        src_ref=part_in.at[others, pl.ds(0, 1)],
        dst_ref=part_in.at[others, pl.ds(0, 1)],
        send_sem=send_sem.at[2, 0],
        recv_sem=recv_sem.at[2, 0, 0],
        device_id={"panel": lax.rem(me + 1, PANELS)},
        device_id_type=MESH,
    )
    shared.wait_recv()
    total = part_in[0, 0:1]
    for k in range(1, PANELS):
        total = total + part_in[k, 0:1]
    sums_ref[0:1] = total
    shared.wait_send()


def finish(mult, rec, sums_ref, prim_hbm, mult_hbm, prim, store_sem):
    for comp in range(2):
        for piece in range(ROWS // 16):
            rows = pl.ds(16 * piece, 16)
            pltpu.make_async_copy(
                mult.at[0, comp, rows], mult_hbm.at[0, comp, rows], store_sem.at[0]
            ).start()
    total = sums_ref[0:1]
    den = total[:, 2:3] + 1e-06
    fit_re = jnp.broadcast_to(total[:, 0:1] / den, (16, 256))
    fit_im = jnp.broadcast_to(total[:, 1:2] / den, (16, 256))
    for piece in range(ROWS // 16):
        rows = slice(16 * piece, 16 * piece + 16)
        for pair in range(WIDTH // 256):
            at = slice(256 * pair, 256 * pair + 256)
            re = mult[0, 0, rows, at].astype(jnp.float32)
            im = mult[0, 1, rows, at].astype(jnp.float32)
            prim[0, 0, rows, at] = rec[0, 0, rows, at] - (fit_re * re - fit_im * im)
            prim[0, 1, rows, at] = rec[0, 1, rows, at] - (fit_re * im + fit_im * re)
        for comp in range(2):
            for part in range(2):
                eight = pl.ds(16 * piece + 8 * part, 8)
                pltpu.make_async_copy(
                    prim.at[0, comp, eight], prim_hbm.at[0, comp, eight], store_sem.at[1]
                ).start()
    pltpu.make_async_copy(mult, mult_hbm, store_sem.at[0]).wait()
    pltpu.make_async_copy(prim, prim_hbm, store_sem.at[1]).wait()


def per_device(*operands):
    vmem = pltpu.VMEM
    bf16 = jnp.bfloat16
    outs = (
        jax.ShapeDtypeStruct((1, 2, ROWS, WIDTH), jnp.float32),
        jax.ShapeDtypeStruct((1, 2, ROWS, WIDTH), bf16),
    )
    held = pl.pallas_call(
        kernel,
        out_shape=(outs[1], outs[0], jax.ShapeDtypeStruct((8, 128), jnp.float32)),
        in_specs=[pl.BlockSpec(memory_space=pltpu.HBM)] * 3,
        out_specs=(pl.BlockSpec(memory_space=vmem),) * 3,
        scratch_shapes=[
            vmem((2, 2, TAPS - 1), bf16),
            vmem((16, TAPS), jnp.float32),
            vmem((2, 128 * (UNITS + 1), 128), bf16),
            vmem((128, TAPS), bf16),
            vmem((2, 128 * UNITS, BLOCK), bf16),
            vmem((2 * ROWS, WIDTH), bf16),
            vmem((2 * ROWS, WIDTH), bf16),
            vmem((4 * SUB, WIDTH + BLOCK), bf16),
            vmem((4 * SUB, WIDTH + BLOCK), bf16),
            vmem((CHUNKS, PANELS, SUB, 128), bf16),
            vmem((CHUNKS, PANELS, SUB, 128), bf16),
            vmem((CHUNKS, PANELS, SUB, 128), bf16),
            vmem((CHUNKS, PANELS, SUB, 128), bf16),
            vmem((1, 8, 128), jnp.float32),
            vmem((PANELS, 8, 128), jnp.float32),
            pltpu.SemaphoreType.DMA((3,)),
            pltpu.SemaphoreType.DMA((3, CHUNKS)),
            pltpu.SemaphoreType.DMA((3, CHUNKS, GROUPS)),
        ],
        compiler_params=pltpu.CompilerParams(
            collective_id=0, has_side_effects=True, vmem_limit_bytes=48 * 1024 * 1024
        ),
    )(*(pltpu.with_memory_space_constraint(x, pltpu.HBM) for x in operands))
    return pl.pallas_call(
        finish,
        out_shape=outs,
        in_specs=[pl.BlockSpec(memory_space=vmem)] * 3,
        out_specs=(pl.BlockSpec(memory_space=pltpu.HBM),) * 2,
        scratch_shapes=[
            vmem((1, 2, ROWS, WIDTH), jnp.float32),
            pltpu.SemaphoreType.DMA((2,)),
        ],
        compiler_params=pltpu.CompilerParams(vmem_limit_bytes=16 * 1024 * 1024),
    )(*held)


def solution(mesh):
    placed = (P("freq", None, "panel", None), P("freq", None, None), P("freq", None, None))
    return jax.shard_map(
        per_device,
        mesh=mesh,
        in_specs=placed,
        out_specs=(P("freq", None, "panel", None), P("freq", None, "panel", None)),
        check_vma=False,
    )
```
